256 devices in a mesh: lat: 8 (over x_lo, y), lon: 32 (over z, x_hi, core).
Axes of the slice: x: 4 (x_hi: 2, x_lo: 2; x = x_hi * 2 + x_lo), y: 4, z: 8, core: 2. Of those that a mesh axis runs over, the one named last changes fastest.
Arguments:
- activations: bfloat16 [4, 32, 2880, 512], P(None, 'lat', 'lon'), may hold values from -48 to 48
- upstream: bfloat16 [4, 32, 2880, 512], P(None, 'lat', 'lon'), may hold values from -6 to 6
- master: float32 [512, 9, 512], P(('lat', 'lon')), may hold values from -0.09375 to 0.09375
- moment_one: float32 [512, 9, 512], P(('lat', 'lon')), may hold values from -2.5 to 2.5
- moment_two: float32 [512, 9, 512], P(('lat', 'lon')), may hold values from 0.01 to 1
Outputs:
- input_grad: bfloat16 [4, 32, 2880, 512], P(None, 'lat', 'lon')
- new_weights: bfloat16 [512, 9, 512], replicated
- new_master: float32 [512, 9, 512], P(('lat', 'lon'))
- new_moment_one: float32 [512, 9, 512], P(('lat', 'lon'))
- new_moment_two: float32 [512, 9, 512], P(('lat', 'lon'))
- clipped_grad: float32 [512, 9, 512], P(('lat', 'lon'))
The draws below stay inside these ranges and needn't reach their ends.
All inputs are finite; a program needn't handle non-finite values.
Results may differ from the reference program's by a relative error of at most 0.0049.
Values may be sent and summed in bfloat16 or wider, within the bound.
No kernel may reach another device: no remote copies, remote signals or barrier semaphores. Data moves between devices by JAX's collectives and lax.ppermute only.
A program may use at most 128 MiB of HBM per device.

```python
import math
import jax
import jax.numpy as jnp
from jax import lax

CIN = 512
COUT = 512
TAPS = 9
BATCH = 4
COLS_DEV = 90
NLAT = 32
NLON = 2880
N_LON = 32


def draw_activations(key, part):
    key_noise, key_spread = jax.random.split(key, 2)
    key_pair = jax.random.fold_in(key, 77)
    channel_ramp = jnp.sqrt(1.0 + 2.0 * jnp.arange(CIN, dtype=jnp.float32) / CIN)
    spread = jnp.exp(jax.random.uniform(key_spread, (CIN,), jnp.float32, 0.0, jnp.log(10.0)))
    chan_scale = channel_ramp * spread / 4.0
    pairing = jax.random.permutation(key_pair, N_LON)
    col_block = jnp.arange(NLON, dtype=jnp.int32) // COLS_DEV
    chan_block = jnp.arange(CIN, dtype=jnp.int32) // (CIN // N_LON)
    heavy = pairing[col_block][:, None] == chan_block[None, :]
    boost = jnp.where(heavy, 6.0, 1.0).astype(jnp.float32)[None, None, :, :]
    noise_draw = jax.random.normal(key_noise, (BATCH, NLAT, NLON, CIN), jnp.float32)
    values = noise_draw * chan_scale * boost
    return jnp.clip(values, -48.0, 48.0).astype(jnp.bfloat16)


def level_of(key, dims, cuts, low, top_value):
    factor_of = 1.0
    for dim, parts in cuts:
        draws = jax.random.uniform(jax.random.fold_in(jax.random.fold_in(key, 6), dim), (parts,), jnp.float32, low / len(cuts), top_value / len(cuts))
        factor_of = factor_of * jnp.repeat(jnp.exp(draws), dims[dim] // parts).reshape((-1,) + (1,) * (len(dims) - 1 - dim))
    return factor_of


def scatter_about(stream_key, extent, deviation, limit, cuts=(), kind=jnp.bfloat16):
    level = level_of(stream_key, extent, cuts, -0.22, 0.18) if cuts else 1.0
    result = jax.random.normal(stream_key, extent, jnp.float32) * deviation * level
    return jnp.minimum(jnp.maximum(result, -limit), limit).astype(kind)


def setup_inputs(seed: int = 0) -> dict:
    key_list = jax.random.split(jax.random.key(seed), 6)
    activations = draw_activations(jax.random.fold_in(key_list[5], 71), 0)
    upstream = scatter_about(key_list[1], (BATCH, NLAT, NLON, COUT), 1.0, 6.0, ((1, 8), (2, 32)))
    master = scatter_about(key_list[2], (CIN, TAPS, COUT), (CIN * TAPS) ** -0.5, 0.09375, ((0, 256),), jnp.float32)
    moment_one = scatter_about(key_list[3], (CIN, TAPS, COUT), 0.3, 2.5, ((0, 256),), jnp.float32)
    moment_two = jnp.clip(jnp.exp(math.log(1.0) - 4.6051702 * jax.random.uniform(key_list[4], (CIN, TAPS, COUT), jnp.float32) ** level_of(key_list[4], (CIN, TAPS, COUT), ((0, 256),), -0.2, 0.2)), 0.01, 1.0)
    return {"activations": activations, "upstream": upstream, "master": master, "moment_one": moment_one, "moment_two": moment_two}


learn_rate = 0.01
beta_one = 0.9
beta_two = 0.999
adam_eps = 1e-08
decay_rate = 0.1
step_count = 10.0
norm_eps = 1e-06

def widen_field(field):
    padded = jnp.pad(field, ((1, 1), (0, 0), (0, 0)))
    return jnp.concatenate([padded[:, -1:, :], padded, padded[:, :1, :]], axis=1)

def reference(activations, upstream, master, moment_one, moment_two):
    weights = master.astype(jnp.bfloat16)

    def one_sample(grad_total, sample):
        act_one, up_one = sample
        act_wide = widen_field(act_one)
        up_wide = widen_field(up_one)
        up_flat = up_one.reshape(-1, COUT)
        data_sum = jnp.zeros((NLAT * NLON, CIN), jnp.float32)
        tap_parts = []
        for tap_index in range(9):
            row_off, col_off = divmod(tap_index, 3)
            shifted = up_wide[2 - row_off:2 - row_off + NLAT, 2 - col_off:2 - col_off + NLON, :].reshape(-1, COUT)
            data_sum = data_sum + jnp.dot(shifted, weights[:, tap_index, :].T, preferred_element_type=jnp.float32)
            act_tap = act_wide[row_off:row_off + NLAT, col_off:col_off + NLON, :].reshape(-1, CIN)
            tap_parts.append(jnp.dot(act_tap.T, up_flat, preferred_element_type=jnp.float32))
        grad_total = grad_total + jnp.stack(tap_parts, axis=1)
        return (grad_total, data_sum.reshape(NLAT, NLON, CIN).astype(jnp.bfloat16))
    grad_total, input_grad = lax.scan(one_sample, jnp.zeros((CIN, 9, COUT), jnp.float32), (activations, upstream))
    max_norm = math.sqrt(float(CIN * TAPS * COUT))
    square_sum = jnp.sum(grad_total * grad_total)
    clip_factor = jnp.minimum(1.0, max_norm / (jnp.sqrt(square_sum) + norm_eps))
    grad_scaled = clip_factor * grad_total
    new_one = beta_one * moment_one + (1.0 - beta_one) * grad_scaled
    new_two = beta_two * moment_two + (1.0 - beta_two) * grad_scaled * grad_scaled
    first_hat = new_one / (1.0 - beta_one ** step_count)
    second_hat = new_two / (1.0 - beta_two ** step_count)
    new_master = master - learn_rate * (first_hat / (jnp.sqrt(second_hat) + adam_eps) + decay_rate * master)
    new_weights = new_master.astype(jnp.bfloat16)
    return (input_grad, new_weights, new_master, new_one, new_two, grad_scaled)
```

```python
import math

import jax
import jax.numpy as jnp
from jax import lax
from jax.experimental import pallas as pl
from jax.experimental.pallas import tpu as pltpu
from jax.sharding import Mesh
from jax.sharding import PartitionSpec as P

TAPS = 9
ALL = ("xl", "y", "z", "xh", "c")
LAT = ("xl", "y")
LON = ("z", "xh", "c")
PLANE = ("xl", "y", "xh")
BF16 = jnp.bfloat16
F32 = jnp.float32

learn_rate = 0.01
beta_one = 0.9
beta_two = 0.999
adam_eps = 1e-08
decay_rate = 0.1
step_count = 10.0
norm_eps = 1e-06


def rows_of(shape, dim):
    return lax.broadcasted_iota(jnp.int32, shape, dim)


def channel_of(core, plane, z, k):
    lat, xh = plane // 2, plane % 2
    return (((lat * 8 + z) * 2 + xh) * 2 + core) * 2 + k


def send_order(p, own_core):
    other, plane, z, k = p // 256, (p // 16) % 16, (p // 2) % 8, p % 2
    return channel_of((other + own_core) % 2, plane, z, k)


def gather_order(p):
    z, core, plane, k = p // 64, (p // 32) % 2, (p // 2) % 16, p % 2
    return channel_of(core, plane, z, k)


def neighbours(count, circular):
    forward = [(i, i + 1) for i in range(count - 1)]
    if circular:
        forward.append((count - 1, 0))
    return forward, [(b, a) for a, b in forward]


def with_halo(rows):
    forward, backward = neighbours(8, False)
    above = lax.ppermute(rows[-1:], LAT, forward)
    below = lax.ppermute(rows[:1], LAT, backward)
    tall = jnp.concatenate([above, rows, below], axis=0)
    forward, backward = neighbours(32, True)
    left = lax.ppermute(tall[:, :, -1:], LON, forward)
    right = lax.ppermute(tall[:, :, :1], LON, backward)
    return left, tall, right


def grad_kernel(lhs_ref, field_ref, keep_ref, send_ref, *, block):
    tap = pl.program_id(0)
    row, col = tap // 3, tap % 3
    start = pl.multiple_of((2 - row) * block, block)
    window = field_ref[col, pl.ds(start, 4 * block), :]
    part = jnp.dot(lhs_ref[...], window, preferred_element_type=F32)
    keep_ref[...] = part[:256]
    send_ref[...] = part[256:].astype(BF16)


def tap_grads(lhs, fields):
    block = fields.shape[1] // 6
    outs = fields.shape[2]
    half = lhs.shape[0] // 2
    return pl.pallas_call(
        lambda *refs: grad_kernel(*refs, block=block),
        grid=(TAPS,),
        in_specs=[
            pl.BlockSpec(lhs.shape, lambda t: (0, 0)),
            pl.BlockSpec(fields.shape, lambda t: (0, 0, 0)),
        ],
        out_specs=[
            pl.BlockSpec((half, outs), lambda t: (0, t)),
            pl.BlockSpec((half, outs), lambda t: (0, t)),
        ],
        out_shape=[
            jax.ShapeDtypeStruct((half, TAPS * outs), F32),
            jax.ShapeDtypeStruct((half, TAPS * outs), BF16),
        ],
        compiler_params=pltpu.CompilerParams(vmem_limit_bytes=48 * 1024 * 1024),
        cost_estimate=pl.CostEstimate(
            flops=2 * lhs.shape[0] * lhs.shape[1] * TAPS * outs,
            bytes_accessed=20_000_000,
            transcendentals=0,
        ),
        name="tap_grads",
    )(lhs, fields)


def pull_kernel(field_ref, weight_ref, order_ref, out_ref, *, block):
    step = pl.program_id(0)
    outs = field_ref.shape[2]
    total = jnp.zeros((block, weight_ref.shape[0]), F32)
    for tap in range(TAPS):
        row, col = divmod(tap, 3)
        start = pl.multiple_of((step + 2 - row) * block, block)
        total = total + lax.dot_general(
            field_ref[col, pl.ds(start, block), :],
            weight_ref[:, tap * outs : (tap + 1) * outs],
            (((1,), (1,)), ((), ())),
            preferred_element_type=F32,
        )
    out_ref[...] = jnp.dot(
        total.astype(BF16), order_ref[...], preferred_element_type=F32
    ).astype(BF16)


def pulled(fields, weights, order):
    block = fields.shape[1] // 6
    chans = weights.shape[0]
    return pl.pallas_call(
        lambda *refs: pull_kernel(*refs, block=block),
        grid=(4,),
        in_specs=[
            pl.BlockSpec(fields.shape, lambda i: (0, 0, 0)),
            pl.BlockSpec(weights.shape, lambda i: (0, 0)),
            pl.BlockSpec(order.shape, lambda i: (0, 0)),
        ],
        out_specs=pl.BlockSpec((block, chans), lambda i: (i, 0)),
        out_shape=jax.ShapeDtypeStruct((4 * block, chans), BF16),
        compiler_params=pltpu.CompilerParams(vmem_limit_bytes=48 * 1024 * 1024),
        cost_estimate=pl.CostEstimate(
            flops=2 * 4 * block * chans * weights.shape[1],
            bytes_accessed=14_000_000,
            transcendentals=0,
        ),
        name="pulled",
    )(fields, weights, order)


def join_kernel(own_ref, other_ref, own_order_ref, other_order_ref, out_ref):
    mine = jnp.dot(own_order_ref[...], own_ref[...], preferred_element_type=F32)
    theirs = jnp.dot(other_order_ref[...], other_ref[...], preferred_element_type=F32)
    out_ref[0] = (mine + theirs).astype(BF16)


def joined(own, other, own_order, other_order):
    half, wide = own.shape
    outs = wide // TAPS
    return pl.pallas_call(
        join_kernel,
        grid=(TAPS,),
        in_specs=[
            pl.BlockSpec((half, outs), lambda t: (0, t)),
            pl.BlockSpec((half, outs), lambda t: (0, t)),
            pl.BlockSpec(own_order.shape, lambda t: (0, 0)),
            pl.BlockSpec(other_order.shape, lambda t: (0, 0)),
        ],
        out_specs=pl.BlockSpec((1, 2 * half, outs), lambda t: (t, 0, 0)),
        out_shape=jax.ShapeDtypeStruct((TAPS, 2 * half, outs), BF16),
        name="joined",
    )(own, other, own_order, other_order)


def to_all(piece, axes, count):
    copies = jnp.broadcast_to(piece[None], (count, *piece.shape))
    return lax.all_to_all(copies, axes, 0, 0, tiled=True)


def per_device(activations, upstream, master, moment_one, moment_two):
    batch, lat_rows, lon_cols, chans = activations.shape
    outs = upstream.shape[3]
    wide = TAPS * outs
    padded_cols = -(-lon_cols // 32) * 32
    extra = padded_cols - lon_cols
    core = lax.axis_index("c")

    old_piece = master.astype(BF16).reshape(2, wide)
    old_plane = to_all(old_piece, PLANE, 16).reshape(32, wide)
    old_weights = lax.all_gather(old_plane, ("z", "c"), axis=0, tiled=True)

    up_rows = jnp.transpose(upstream, (1, 0, 2, 3))
    left, tall, right = with_halo(up_rows)
    filler = jnp.zeros((6, batch, extra, outs), BF16)
    field = jnp.concatenate([left, tall, right, filler], axis=2)
    fields = jnp.stack(
        [field[:, :, 2 - s : 2 - s + padded_cols].reshape(-1, outs) for s in range(3)]
    )

    square = (chans, chans)
    act_rows = jnp.pad(
        jnp.transpose(activations, (1, 0, 2, 3)), ((0, 0), (0, 0), (0, extra), (0, 0))
    ).reshape(-1, chans)
    order = (send_order(rows_of(square, 0), core) == rows_of(square, 1)).astype(BF16)
    lhs = lax.dot_general(
        order, act_rows, (((1,), (1,)), ((), ())), preferred_element_type=F32
    ).astype(BF16)

    keep, send = tap_grads(lhs, fields)
    swapped = lax.ppermute(send, "c", [(0, 1), (1, 0)])
    pair_sum = (keep + swapped.astype(F32)).astype(BF16).reshape(16, 16, wide)
    parts = lax.all_to_all(pair_sum, PLANE, 0, 0, tiled=True)
    plane_sum = jnp.sum(parts.astype(F32), axis=0).astype(BF16).reshape(8, 2, wide)
    parts = lax.all_to_all(plane_sum, ("z",), 0, 0, tiled=True)
    grad = jnp.sum(parts.astype(F32), axis=0).reshape(2, TAPS, outs)

    square_sum = jnp.sum(grad * grad).reshape(1, 1, 1)
    square_sum = jnp.sum(to_all(square_sum.reshape(1, 1), PLANE, 16)).reshape(1, 1)
    square_sum = jnp.sum(to_all(square_sum, ("z", "c"), 16))
    max_norm = math.sqrt(float(chans * TAPS * outs))
    clip_factor = jnp.minimum(1.0, max_norm / (jnp.sqrt(square_sum) + norm_eps))
    clipped = clip_factor * grad
    new_one = beta_one * moment_one + (1.0 - beta_one) * clipped
    new_two = beta_two * moment_two + (1.0 - beta_two) * clipped * clipped
    first_hat = new_one / (1.0 - beta_one**step_count)
    second_hat = new_two / (1.0 - beta_two**step_count)
    new_master = master - learn_rate * (
        first_hat / (jnp.sqrt(second_hat) + adam_eps) + decay_rate * master
    )

    new_piece = new_master.astype(BF16).reshape(2, wide)
    line = to_all(new_piece, ("z",), 8).reshape(16, wide)
    own = to_all(line, PLANE, 16).reshape(256, wide)
    other = lax.ppermute(own, "c", [(0, 1), (1, 0)])
    half = (chans, chans // 2)
    picked = [
        (send_order(rows_of(half, 1) + 256 * i, core) == rows_of(half, 0)).astype(BF16)
        for i in range(2)
    ]
    new_weights = jnp.transpose(joined(own, other, *picked), (1, 0, 2))

    back = (gather_order(rows_of(square, 0)) == rows_of(square, 1)).astype(BF16)
    pulled_rows = pulled(fields, old_weights, back)
    input_grad = pulled_rows.reshape(lat_rows, batch, padded_cols, chans)[:, :, :lon_cols]
    input_grad = jnp.transpose(input_grad, (1, 0, 2, 3))
    return (input_grad, new_weights, new_master, new_one, new_two, clipped)


def solution(mesh):
    split = Mesh(mesh.devices.reshape(2, 4, 8, 2, 2), ALL)
    field = P(None, LAT, LON, None)
    state = P(ALL, None, None)
    return jax.shard_map(
        per_device,
        mesh=split,
        in_specs=(field, field, state, state, state),
        out_specs=(field, P(), state, state, state, state),
        check_vma=False,
    )
```

```python
import math

import jax
import jax.numpy as jnp
from jax import lax
from jax.experimental import pallas as pl
from jax.experimental.pallas import tpu as pltpu
from jax.sharding import Mesh
from jax.sharding import PartitionSpec as P


TAPS = 9
ALL = ("xl", "y", "z", "xh", "c")
LAT = ("xl", "y")
LON = ("z", "xh", "c")
PLANE = ("xl", "y", "xh")
BF16 = jnp.bfloat16
F32 = jnp.float32

learn_rate = 0.01
beta_one = 0.9
beta_two = 0.999
adam_eps = 1e-08
decay_rate = 0.1
step_count = 10.0
norm_eps = 1e-06


def rows_of(shape, dim):
    return lax.broadcasted_iota(jnp.int32, shape, dim)


def channel_of(core, plane, z, k):
    lat, xh = plane // 2, plane % 2
    return (((lat * 8 + z) * 2 + xh) * 2 + core) * 2 + k


def gather_order(p):
    z, core, plane, k = p // 64, (p // 32) % 2, (p // 2) % 16, p % 2
    return channel_of(core, plane, z, k)


def neighbours(count, circular):
    forward = [(i, i + 1) for i in range(count - 1)]
    if circular:
        forward.append((count - 1, 0))
    return forward, [(b, a) for a, b in forward]


def row_halo(rows):
    forward, backward = neighbours(8, False)
    above = lax.ppermute(rows[-1:], LAT, forward)
    below = lax.ppermute(rows[:1], LAT, backward)
    return above, below


def col_halo(above, rows, below):
    east = jnp.concatenate([part[:, :, -1:] for part in (above, rows, below)], axis=0)
    west = jnp.concatenate([part[:, :, :1] for part in (above, rows, below)], axis=0)
    forward, backward = neighbours(32, True)
    left = lax.ppermute(east, LON, forward)
    right = lax.ppermute(west, LON, backward)
    return left, right


def swap(array):
    return lax.ppermute(array, "c", [(0, 1), (1, 0)])


def store_halves(core_ref, lhs, window_of, keep_ref, send_ref):
    half = keep_ref.shape[1]
    own = pl.multiple_of(core_ref[0] * half, half)
    other = pl.multiple_of((1 - core_ref[0]) * half, half)
    send_ref[...] = window_of(lhs, pl.ds(other, half)).astype(BF16)
    keep_ref[...] = window_of(lhs, pl.ds(own, half))


def centre_kernel(core_ref, lhs_ref, above_ref, rows_ref, below_ref, keep_ref, send_ref):
    block = above_ref.shape[0]
    row = pl.program_id(0)

    def dots(pieces, outs):
        total = None
        for start, ref, first, count in pieces:
            part = jnp.dot(
                lhs_ref[:, start : start + count],
                ref[first : first + count, outs],
                preferred_element_type=F32,
            )
            total = part if total is None else total + part
        return total

    plans = (
        ((0, rows_ref, block, 3 * block), (3 * block, below_ref, 0, block)),
        ((0, rows_ref, 0, 4 * block),),
        ((0, above_ref, 0, block), (block, rows_ref, 0, 3 * block)),
    )
    for index, plan in enumerate(plans):

        @pl.when(row == index)
        def _(plan=plan):
            store_halves(core_ref, None, lambda _, outs: dots(plan, outs), keep_ref, send_ref)


def centre_grads(core, lhs, above, rows, below):
    chans, outs = lhs.shape[0], rows.shape[1]
    half = outs // 2
    whole = lambda array: pl.BlockSpec(array.shape, lambda t: (0,) * array.ndim)
    return pl.pallas_call(
        centre_kernel,
        grid=(3,),
        in_specs=[
            pl.BlockSpec(memory_space=pltpu.SMEM),
            whole(lhs),
            whole(above),
            whole(rows),
            whole(below),
        ],
        out_specs=[pl.BlockSpec((chans, half), lambda t: (0, t))] * 2,
        out_shape=[
            jax.ShapeDtypeStruct((chans, 3 * half), F32),
            jax.ShapeDtypeStruct((chans, 3 * half), BF16),
        ],
        compiler_params=pltpu.CompilerParams(vmem_limit_bytes=48 * 1024 * 1024),
        cost_estimate=pl.CostEstimate(
            flops=2 * chans * lhs.shape[1] * 3 * outs, bytes_accessed=8_000_000, transcendentals=0
        ),
        name="centre_grads",
    )(core, lhs, above, rows, below)


def side_kernel(
    core_ref, lhs_ref, above_ref, rows_ref, below_ref, left_ref, right_ref,
    field_ref, keep_ref, send_ref, *, cols, padded_cols,
):
    step = pl.program_id(0)
    block = above_ref.shape[0]
    batch = block // padded_cols

    @pl.when(step == 0)
    def _():
        index = lax.broadcasted_iota(jnp.int32, (padded_cols, 1), 0)
        for line in range(6 * batch):
            first = line * padded_cols
            if line < batch:
                ref, start = above_ref, first
            elif line < 5 * batch:
                ref, start = rows_ref, first - block
            else:
                ref, start = below_ref, first - 5 * block
            centre = ref[start : start + padded_cols, :]
            field_ref[1, first : first + padded_cols, :] = centre
            wide = centre.astype(F32)
            east = pltpu.roll(wide, padded_cols - 1, 0)
            east = jnp.where(index == cols - 1, right_ref[line : line + 1, :], east)
            field_ref[0, first : first + padded_cols, :] = east.astype(BF16)
            west = pltpu.roll(wide, 1, 0)
            west = jnp.where(index == 0, left_ref[line : line + 1, :], west)
            field_ref[2, first : first + padded_cols, :] = west.astype(BF16)

    row, side = step // 2, 2 * (step % 2)
    start = pl.multiple_of((2 - row) * block, block)

    def window_dot(_, outs):
        return jnp.dot(
            lhs_ref[...],
            field_ref[side, pl.ds(start, 4 * block), outs],
            preferred_element_type=F32,
        )

    store_halves(core_ref, None, window_dot, keep_ref, send_ref)


def side_grads(core, lhs, above, rows, below, left, right, cols, padded_cols):
    chans, outs = lhs.shape[0], rows.shape[1]
    half = outs // 2
    whole = lambda array: pl.BlockSpec(array.shape, lambda t: (0,) * array.ndim)
    length = rows.shape[0] * 3 // 2
    return pl.pallas_call(
        lambda *refs: side_kernel(*refs, cols=cols, padded_cols=padded_cols),
        grid=(6,),
        in_specs=[pl.BlockSpec(memory_space=pltpu.SMEM)]
        + [whole(array) for array in (lhs, above, rows, below, left, right)],
        out_specs=[pl.BlockSpec((3, length, outs), lambda t: (0, 0, 0))]
        + [pl.BlockSpec((chans, half), lambda t: (0, t))] * 2,
        out_shape=[
            jax.ShapeDtypeStruct((3, length, outs), BF16),
            jax.ShapeDtypeStruct((chans, 6 * half), F32),
            jax.ShapeDtypeStruct((chans, 6 * half), BF16),
        ],
        compiler_params=pltpu.CompilerParams(vmem_limit_bytes=56 * 1024 * 1024),
        cost_estimate=pl.CostEstimate(
            flops=2 * chans * lhs.shape[1] * 6 * outs, bytes_accessed=16_000_000, transcendentals=0
        ),
        name="side_grads",
    )(core, lhs, above, rows, below, left, right)


def pull_kernel(field_ref, weight_ref, order_ref, out_ref, *, block):
    step = pl.program_id(0)
    outs = field_ref.shape[2]
    total = jnp.zeros((block, weight_ref.shape[0]), F32)
    for tap in range(TAPS):
        row, col = divmod(tap, 3)
        start = pl.multiple_of((step + 2 - row) * block, block)
        total = total + lax.dot_general(
            field_ref[col, pl.ds(start, block), :],
            weight_ref[:, tap * outs : (tap + 1) * outs],
            (((1,), (1,)), ((), ())),
            preferred_element_type=F32,
        )
    out_ref[...] = jnp.dot(
        total.astype(BF16), order_ref[...], preferred_element_type=F32
    ).astype(BF16)


def pulled(fields, weights, order):
    block = fields.shape[1] // 6
    chans = weights.shape[0]
    return pl.pallas_call(
        lambda *refs: pull_kernel(*refs, block=block),
        grid=(4,),
        in_specs=[
            pl.BlockSpec(fields.shape, lambda i: (0, 0, 0)),
            pl.BlockSpec(weights.shape, lambda i: (0, 0)),
            pl.BlockSpec(order.shape, lambda i: (0, 0)),
        ],
        out_specs=pl.BlockSpec((block, chans), lambda i: (i, 0)),
        out_shape=jax.ShapeDtypeStruct((4 * block, chans), BF16),
        compiler_params=pltpu.CompilerParams(vmem_limit_bytes=48 * 1024 * 1024),
        cost_estimate=pl.CostEstimate(
            flops=2 * 4 * block * chans * weights.shape[1],
            bytes_accessed=14_000_000,
            transcendentals=0,
        ),
        name="pulled",
    )(fields, weights, order)


def join_kernel(core_ref, own_ref, other_ref, out_ref):
    half = own_ref.shape[1]
    own = pl.multiple_of(core_ref[0] * half, half)
    other = pl.multiple_of((1 - core_ref[0]) * half, half)
    out_ref[0, :, pl.ds(own, half)] = own_ref[...]
    out_ref[0, :, pl.ds(other, half)] = other_ref[...]


def joined(core, own, other):
    chans, wide = own.shape
    half = wide // TAPS
    return pl.pallas_call(
        join_kernel,
        grid=(TAPS,),
        in_specs=[
            pl.BlockSpec(memory_space=pltpu.SMEM),
            pl.BlockSpec((chans, half), lambda t: (0, t)),
            pl.BlockSpec((chans, half), lambda t: (0, t)),
        ],
        out_specs=pl.BlockSpec((1, chans, 2 * half), lambda t: (t, 0, 0)),
        out_shape=jax.ShapeDtypeStruct((TAPS, chans, 2 * half), BF16),
        name="joined",
    )(core, own, other)


def to_all(piece, axes, count):
    copies = jnp.broadcast_to(piece[None], (count, *piece.shape))
    return lax.all_to_all(copies, axes, 0, 0, tiled=True)


def halves(array, core):
    half = array.shape[-1] // 2
    low, high = array[..., :half], array[..., half:]
    return jnp.where(core == 0, low, high), jnp.where(core == 0, high, low)


def in_core_order(own, other, core, axis):
    return jnp.where(
        core == 0,
        jnp.concatenate([own, other], axis=axis),
        jnp.concatenate([other, own], axis=axis),
    )


def per_device(activations, upstream, master, moment_one, moment_two):
    batch, lat_rows, lon_cols, chans = activations.shape
    outs = upstream.shape[3]
    wide = TAPS * outs
    half = outs // 2
    padded_cols = -(-lon_cols // 32) * 32
    extra = padded_cols - lon_cols
    core = lax.axis_index("c")
    core_ref = core.reshape(1).astype(jnp.int32)

    def padded(rows):
        return jnp.pad(rows, ((0, 0), (0, 0), (0, extra), (0, 0))).reshape(-1, rows.shape[3])

    up_rows = jnp.transpose(upstream, (1, 0, 2, 3))
    above, below = row_halo(up_rows)

    old_piece = master.astype(BF16).reshape(2, wide)
    old_plane = to_all(old_piece, PLANE, 16).reshape(32, wide)
    state = jnp.stack([master, moment_one, moment_two])
    own_state, other_state = halves(state, core)
    state = in_core_order(own_state, swap(other_state), core, 1)
    above, below, old_plane, state = lax.optimization_barrier((above, below, old_plane, state))
    old_weights = lax.all_gather(old_plane, ("z", "c"), axis=0, tiled=True)

    left, right = col_halo(above, up_rows, below)
    lhs = padded(jnp.transpose(activations, (1, 0, 2, 3))).T
    pieces = (padded(above), padded(up_rows), padded(below))
    keep_one, send_one = centre_grads(core_ref, lhs, *pieces)
    swapped_one = swap(send_one)
    left, right, keep_one = lax.optimization_barrier((left, right, keep_one))
    sides = [side.reshape(-1, outs).astype(F32) for side in (left, right)]
    fields, keep_two, send_two = side_grads(core_ref, lhs, *pieces, *sides, lon_cols, padded_cols)
    swapped_two = swap(send_two)
    pair_sum = jnp.concatenate(
        [
            (keep_one + swapped_one.astype(F32)).astype(BF16),
            (keep_two + swapped_two.astype(F32)).astype(BF16),
        ],
        axis=1,
    ).reshape(8, 64, TAPS * half)
    parts = lax.all_to_all(pair_sum, LAT, 0, 0, tiled=True)
    lat_sum = jnp.sum(parts.astype(F32), axis=0).astype(BF16).reshape(16, 4, TAPS * half)
    parts = lax.all_to_all(lat_sum, ("z", "xh"), 0, 0, tiled=True)
    grad = jnp.sum(parts.astype(F32), axis=0).reshape(4, TAPS, half)
    square_sum = jnp.sum(grad * grad).reshape(1, 1)
    centre, sides = grad[:, :3], grad[:, 3:].reshape(4, 3, 2, half)
    grad = jnp.stack([sides[:, :, 0], centre, sides[:, :, 1]], axis=2).reshape(4, TAPS, half)

    square_sum = jnp.sum(to_all(square_sum, PLANE, 16)).reshape(1, 1)
    square_sum = jnp.sum(to_all(square_sum, ("z", "c"), 16))
    max_norm = math.sqrt(float(chans * TAPS * outs))
    clip_factor = jnp.minimum(1.0, max_norm / (jnp.sqrt(square_sum) + norm_eps))
    clipped = clip_factor * grad
    old_master, old_one, old_two = state
    new_one = beta_one * old_one + (1.0 - beta_one) * clipped
    new_two = beta_two * old_two + (1.0 - beta_two) * clipped * clipped
    first_hat = new_one / (1.0 - beta_one**step_count)
    second_hat = new_two / (1.0 - beta_two**step_count)
    new_master = old_master - learn_rate * (
        first_hat / (jnp.sqrt(second_hat) + adam_eps) + decay_rate * old_master
    )

    new_piece = new_master.astype(BF16).reshape(4, TAPS * half)
    line = to_all(new_piece, ("z", "xh"), 16).reshape(64, TAPS * half)
    line, fields, old_weights, results = lax.optimization_barrier(
        (line, fields, old_weights, jnp.stack([new_master, new_one, new_two, clipped]))
    )
    own = to_all(line, LAT, 8).reshape(chans, TAPS * half)
    mine = jnp.where(core == 0, results[:, :2], results[:, 2:])
    theirs = jnp.where(core == 0, results[:, 2:], results[:, :2])
    results = in_core_order(mine, swap(theirs), core, 3)

    square = (chans, chans)
    back = (gather_order(rows_of(square, 0)) == rows_of(square, 1)).astype(BF16)
    pulled_rows = pulled(fields, old_weights, back)
    input_grad = pulled_rows.reshape(lat_rows, batch, padded_cols, chans)[:, :, :lon_cols]
    input_grad = jnp.transpose(input_grad, (1, 0, 2, 3))

    new_weights = jnp.transpose(joined(core_ref, own, swap(own)), (1, 0, 2))
    return (input_grad, new_weights, *results)


def solution(mesh):
    split = Mesh(mesh.devices.reshape(2, 4, 8, 2, 2), ALL)
    field = P(None, LAT, LON, None)
    state = P(ALL, None, None)
    return jax.shard_map(
        per_device,
        mesh=split,
        in_specs=(field, field, state, state, state),
        out_specs=(field, P(), state, state, state, state),
        check_vma=False,
    )
```

```python
import math

import jax
import jax.numpy as jnp
from jax import lax
from jax.experimental import pallas as pl
from jax.experimental.pallas import tpu as pltpu
from jax.sharding import Mesh
from jax.sharding import PartitionSpec as P


TAPS = 9
ORDER = (1, 4, 7, 0, 2, 3, 5, 6, 8)
ALL = ("xl", "y", "z", "xh", "c")
LAT = ("xl", "y")
LON = ("z", "xh", "c")
PLANE = ("xl", "y", "xh")
BF16 = jnp.bfloat16
F32 = jnp.float32

learn_rate = 0.01
beta_one = 0.9
beta_two = 0.999
adam_eps = 1e-08
decay_rate = 0.1
step_count = 10.0
norm_eps = 1e-06


def rows_of(shape, dim):
    return lax.broadcasted_iota(jnp.int32, shape, dim)


def channel_of(core, plane, z, k):
    lat, xh = plane // 2, plane % 2
    return (((lat * 8 + z) * 2 + xh) * 2 + core) * 2 + k


def gather_order(p):
    z, core, plane, k = p // 64, (p // 32) % 2, (p // 2) % 16, p % 2
    return channel_of(core, plane, z, k)


def row_channel(p):
    plane, z, rest = p // 32, (p // 4) % 8, p % 4
    return channel_of(rest // 2, plane, z, rest % 2)


def neighbours(count, circular):
    forward = [(i, i + 1) for i in range(count - 1)]
    if circular:
        forward.append((count - 1, 0))
    return forward, [(b, a) for a, b in forward]


def row_halo(first, last):
    forward, backward = neighbours(8, False)
    return lax.ppermute(last, LAT, forward), lax.ppermute(first, LAT, backward)


def col_halo(parts, last_col):
    east = jnp.concatenate([part[:, :, last_col : last_col + 1] for part in parts], axis=0)
    west = jnp.concatenate([part[:, :, :1] for part in parts], axis=0)
    forward, backward = neighbours(32, True)
    return lax.ppermute(east, LON, forward), lax.ppermute(west, LON, backward)


def swap(array):
    return lax.ppermute(array, "c", [(0, 1), (1, 0)])


def store_halves(core_ref, lhs, window_of, keep_ref, send_ref):
    half = keep_ref.shape[1]
    own = pl.multiple_of(core_ref[0] * half, half)
    other = pl.multiple_of((1 - core_ref[0]) * half, half)
    send_ref[...] = window_of(lhs, pl.ds(other, half)).astype(BF16)
    keep_ref[...] = window_of(lhs, pl.ds(own, half))


def centre_kernel(core_ref, lhs_ref, above_ref, rows_ref, below_ref, keep_ref, send_ref):
    block = above_ref.shape[0]
    row = pl.program_id(0)

    def dots(pieces, outs):
        total = None
        for start, ref, first, count in pieces:
            part = jnp.dot(
                lhs_ref[:, start : start + count],
                ref[first : first + count, outs],
                preferred_element_type=F32,
            )
            total = part if total is None else total + part
        return total

    plans = (
        ((0, rows_ref, block, 3 * block), (3 * block, below_ref, 0, block)),
        ((0, rows_ref, 0, 4 * block),),
        ((0, above_ref, 0, block), (block, rows_ref, 0, 3 * block)),
    )
    for index, plan in enumerate(plans):

        @pl.when(row == index)
        def _(plan=plan):
            store_halves(core_ref, None, lambda _, outs: dots(plan, outs), keep_ref, send_ref)


def centre_grads(core, lhs, above, rows, below):
    chans, outs = lhs.shape[0], rows.shape[1]
    half = outs // 2
    whole = lambda array: pl.BlockSpec(array.shape, lambda t: (0,) * array.ndim)
    return pl.pallas_call(
        centre_kernel,
        grid=(3,),
        in_specs=[
            pl.BlockSpec(memory_space=pltpu.SMEM),
            whole(lhs),
            whole(above),
            whole(rows),
            whole(below),
        ],
        out_specs=[pl.BlockSpec((chans, half), lambda t: (0, t))] * 2,
        out_shape=[
            jax.ShapeDtypeStruct((chans, 3 * half), F32),
            jax.ShapeDtypeStruct((chans, 3 * half), BF16),
        ],
        compiler_params=pltpu.CompilerParams(vmem_limit_bytes=48 * 1024 * 1024),
        cost_estimate=pl.CostEstimate(
            flops=2 * chans * lhs.shape[1] * 3 * outs, bytes_accessed=8_000_000, transcendentals=0
        ),
        name="centre_grads",
    )(core, lhs, above, rows, below)


def side_kernel(
    core_ref, lhs_ref, above_ref, rows_ref, below_ref, left_ref, right_ref,
    field_ref, keep_ref, send_ref, *, cols, padded_cols,
):
    step = pl.program_id(0)
    block = above_ref.shape[0]
    batch = block // padded_cols

    @pl.when(step == 0)
    def _():
        index = lax.broadcasted_iota(jnp.int32, (padded_cols, 1), 0)
        for line in range(6 * batch):
            first = line * padded_cols
            if line < batch:
                ref, start = above_ref, first
            elif line < 5 * batch:
                ref, start = rows_ref, first - block
            else:
                ref, start = below_ref, first - 5 * block
            centre = ref[start : start + padded_cols, :]
            field_ref[1, first : first + padded_cols, :] = centre
            wide = centre.astype(F32)
            east = pltpu.roll(wide, padded_cols - 1, 0)
            east = jnp.where(index == cols - 1, right_ref[line // batch, line % batch].astype(F32), east)
            field_ref[0, first : first + padded_cols, :] = east.astype(BF16)
            west = pltpu.roll(wide, 1, 0)
            west = jnp.where(index == 0, left_ref[line // batch, line % batch].astype(F32), west)
            field_ref[2, first : first + padded_cols, :] = west.astype(BF16)

    row, side = step // 2, 2 * (step % 2)
    start = pl.multiple_of((2 - row) * block, block)

    def window_dot(_, outs):
        return jnp.dot(
            lhs_ref[...],
            field_ref[side, pl.ds(start, 4 * block), outs],
            preferred_element_type=F32,
        )

    store_halves(core_ref, None, window_dot, keep_ref, send_ref)


def side_grads(core, lhs, above, rows, below, left, right, cols, padded_cols):
    chans, outs = lhs.shape[0], rows.shape[1]
    half = outs // 2
    whole = lambda array: pl.BlockSpec(array.shape, lambda t: (0,) * array.ndim)
    length = rows.shape[0] * 3 // 2
    return pl.pallas_call(
        lambda *refs: side_kernel(*refs, cols=cols, padded_cols=padded_cols),
        grid=(6,),
        in_specs=[pl.BlockSpec(memory_space=pltpu.SMEM)]
        + [whole(array) for array in (lhs, above, rows, below, left, right)],
        out_specs=[pl.BlockSpec((3, length, outs), lambda t: (0, 0, 0))]
        + [pl.BlockSpec((chans, half), lambda t: (0, t))] * 2,
        out_shape=[
            jax.ShapeDtypeStruct((3, length, outs), BF16),
            jax.ShapeDtypeStruct((chans, 6 * half), F32),
            jax.ShapeDtypeStruct((chans, 6 * half), BF16),
        ],
        compiler_params=pltpu.CompilerParams(vmem_limit_bytes=56 * 1024 * 1024),
        cost_estimate=pl.CostEstimate(
            flops=2 * chans * lhs.shape[1] * 6 * outs, bytes_accessed=16_000_000, transcendentals=0
        ),
        name="side_grads",
    )(core, lhs, above, rows, below, left, right)


def pull_kernel(field_ref, weight_ref, order_ref, out_ref, *, block):
    step = pl.program_id(0)
    outs = field_ref.shape[2]
    total = jnp.zeros((block, weight_ref.shape[0]), F32)
    for tap in range(TAPS):
        row, col = divmod(tap, 3)
        start = pl.multiple_of((step + 2 - row) * block, block)
        total = total + lax.dot_general(
            field_ref[col, pl.ds(start, block), :],
            weight_ref[:, tap * outs : (tap + 1) * outs],
            (((1,), (1,)), ((), ())),
            preferred_element_type=F32,
        )
    out_ref[...] = jnp.dot(
        total.astype(BF16), order_ref[...], preferred_element_type=F32
    ).astype(BF16)


def pulled(fields, weights, order):
    block = fields.shape[1] // 6
    chans = weights.shape[0]
    return pl.pallas_call(
        lambda *refs: pull_kernel(*refs, block=block),
        grid=(4,),
        in_specs=[
            pl.BlockSpec(fields.shape, lambda i: (0, 0, 0)),
            pl.BlockSpec(weights.shape, lambda i: (0, 0)),
            pl.BlockSpec(order.shape, lambda i: (0, 0)),
        ],
        out_specs=pl.BlockSpec((block, chans), lambda i: (i, 0)),
        out_shape=jax.ShapeDtypeStruct((4 * block, chans), BF16),
        compiler_params=pltpu.CompilerParams(vmem_limit_bytes=48 * 1024 * 1024),
        cost_estimate=pl.CostEstimate(
            flops=2 * 4 * block * chans * weights.shape[1],
            bytes_accessed=14_000_000,
            transcendentals=0,
        ),
        name="pulled",
    )(fields, weights, order)


def adam_kernel(sums_ref, grad_ref, master_ref, one_ref, two_ref, out_ref, *, max_norm):
    clip = clip_factor(jnp.sum(sums_ref[...], keepdims=True), max_norm)
    state = adam(clip, grad_ref[...], master_ref[...], one_ref[...], two_ref[...])
    out_ref[...] = state[0].astype(BF16)


def clip_factor(square_sum, max_norm):
    return jnp.minimum(1.0, max_norm / (jnp.sqrt(square_sum) + norm_eps))


def adam(clip, grad, master, moment_one, moment_two):
    clipped = clip * grad
    new_one = beta_one * moment_one + (1.0 - beta_one) * clipped
    new_two = beta_two * moment_two + (1.0 - beta_two) * clipped * clipped
    first_hat = new_one / (1.0 - beta_one**step_count)
    second_hat = new_two / (1.0 - beta_two**step_count)
    new_master = master - learn_rate * (
        first_hat / (jnp.sqrt(second_hat) + adam_eps) + decay_rate * master
    )
    return new_master, new_one, new_two, clipped


def stepped(sums, grad, state, max_norm):
    return pl.pallas_call(
        lambda *refs: adam_kernel(*refs, max_norm=max_norm),
        out_shape=jax.ShapeDtypeStruct(grad.shape, BF16),
        cost_estimate=pl.CostEstimate(
            flops=20 * grad.size, bytes_accessed=18 * grad.size, transcendentals=0
        ),
        name="stepped",
    )(sums, grad, *state)


def join_kernel(core_ref, order_ref, own_ref, other_ref, out_ref):
    half = own_ref.shape[1] // TAPS
    own = pl.multiple_of(core_ref[0] * half, half)
    other = pl.multiple_of((1 - core_ref[0]) * half, half)
    for lane, ref in ((own, own_ref), (other, other_ref)):
        rows = jnp.dot(order_ref[...], ref[...], preferred_element_type=F32).astype(BF16)
        for index, tap in enumerate(ORDER):
            out_ref[tap, :, pl.ds(lane, half)] = rows[:, index * half : (index + 1) * half]


def joined(core, order, own, other):
    chans, wide = own.shape
    half = wide // TAPS
    block = order.shape[0]
    return pl.pallas_call(
        join_kernel,
        grid=(chans // block,),
        in_specs=[
            pl.BlockSpec(memory_space=pltpu.SMEM),
            pl.BlockSpec(order.shape, lambda i: (0, 0)),
            pl.BlockSpec((block, wide), lambda i: (i, 0)),
            pl.BlockSpec((block, wide), lambda i: (i, 0)),
        ],
        out_specs=pl.BlockSpec((TAPS, block, 2 * half), lambda i: (0, i, 0)),
        out_shape=jax.ShapeDtypeStruct((TAPS, chans, 2 * half), BF16),
        name="joined",
    )(core, order, own, other)


def to_all(piece, axes, count):
    copies = jnp.broadcast_to(piece[None], (count, *piece.shape))
    return lax.all_to_all(copies, axes, 0, 0, tiled=True)


def halves(array, core):
    half = array.shape[-1] // 2
    low, high = array[..., :half], array[..., half:]
    return jnp.where(core == 0, low, high), jnp.where(core == 0, high, low)


def in_core_order(own, other, core, axis):
    return jnp.where(
        core == 0,
        jnp.concatenate([own, other], axis=axis),
        jnp.concatenate([other, own], axis=axis),
    )


def per_device(activations, upstream, master, moment_one, moment_two):
    batch, lat_rows, lon_cols, chans = activations.shape
    outs = upstream.shape[3]
    half = outs // 2
    wide = TAPS * half
    padded_cols = -(-lon_cols // 32) * 32
    extra = padded_cols - lon_cols
    core = lax.axis_index("c")
    core_ref = core.reshape(1).astype(jnp.int32)
    square = (chans, chans)

    def padded(field):
        return jnp.pad(
            jnp.transpose(field, (1, 0, 2, 3)), ((0, 0), (0, 0), (0, extra), (0, 0))
        )

    def flat(rows):
        return rows.reshape(-1, rows.shape[3])

    above, below = row_halo(padded(upstream[:, :1]), padded(upstream[:, -1:]))
    up_rows = padded(upstream)
    order = (row_channel(rows_of(square, 0)) == rows_of(square, 1)).astype(BF16)
    lhs = lax.dot_general(
        order, flat(padded(activations)), (((1,), (1,)), ((), ())), preferred_element_type=F32
    ).astype(BF16)
    state = jnp.stack([master, moment_one, moment_two])
    own_state, other_state = halves(state, core)
    other_state = swap(other_state)
    state = in_core_order(own_state, other_state, core, 1)
    state = jnp.stack([state[:, :, tap] for tap in ORDER], axis=2).reshape(12, wide)
    lines = lax.all_gather(jnp.pad(state, ((0, 4), (0, 0))), ("z",), axis=0, tiled=True)

    left, right = col_halo((above, up_rows, below), lon_cols - 1)
    pieces = (flat(above), flat(up_rows), flat(below))
    old_piece = master.astype(BF16).reshape(2, TAPS * outs)
    old_plane = to_all(old_piece, PLANE, 16).reshape(32, TAPS * outs)
    old_weights = lax.all_gather(old_plane, ("z", "c"), axis=0, tiled=True)
    keep_one, send_one = centre_grads(core_ref, lhs, *pieces)
    swapped_one = swap(send_one)
    left, right, keep_one = lax.optimization_barrier((left, right, keep_one))
    fields, keep_two, send_two = side_grads(
        core_ref, lhs, *pieces, left, right, lon_cols, padded_cols
    )
    swapped_two = swap(send_two)
    pair_sum = jnp.concatenate(
        [
            (keep_one + swapped_one.astype(F32)).astype(BF16),
            (keep_two + swapped_two.astype(F32)).astype(BF16),
        ],
        axis=1,
    ).reshape(16, 32, wide)
    parts = lax.all_to_all(pair_sum, PLANE, 0, 0, tiled=True)
    lines = lines.reshape(8, 4, 4, wide)
    lines = [lines[:, i].reshape(32, wide) for i in range(3)]
    plane_sum = jnp.sum(parts.astype(F32), axis=0).astype(BF16).reshape(8, 4, wide)
    parts = lax.all_to_all(plane_sum, ("z",), 0, 0, tiled=True)
    grad = jnp.sum(parts.astype(F32), axis=0)
    grad_line = to_all(grad, ("z",), 8).reshape(32, wide)

    square_sum = jnp.sum(grad_line * grad_line).reshape(1, 1)
    sums = to_all(square_sum, PLANE + ("c",), 32).reshape(1, 32)
    max_norm = math.sqrt(float(chans * TAPS * outs))
    new_line = stepped(sums, grad_line, lines, max_norm)
    own = to_all(new_line, PLANE, 16).reshape(chans, wide)

    clip = clip_factor(jnp.sum(sums).reshape(1, 1), max_norm)
    results = jnp.stack(adam(clip, grad, *state.reshape(3, 4, wide)))
    results = results.reshape(4, 4, TAPS, half)
    results = jnp.stack([results[:, :, ORDER.index(tap)] for tap in range(TAPS)], axis=2)
    mine = jnp.where(core == 0, results[:, :2], results[:, 2:])
    theirs = jnp.where(core == 0, results[:, 2:], results[:, :2])
    results = in_core_order(mine, swap(theirs), core, 3)

    fields, old_weights, _ = lax.optimization_barrier((fields, old_weights, new_line))
    old_order = (gather_order(rows_of(square, 0)) == rows_of(square, 1)).astype(BF16)
    pulled_rows = pulled(fields, old_weights, old_order)
    input_grad = pulled_rows.reshape(lat_rows, batch, padded_cols, chans)[:, :, :lon_cols]
    input_grad = jnp.transpose(input_grad, (1, 0, 2, 3))

    lat_block = (chans // 8, chans // 8)
    back = (rows_of(lat_block, 0) == row_channel(rows_of(lat_block, 1))).astype(BF16)
    new_weights = jnp.transpose(joined(core_ref, back, own, swap(own)), (1, 0, 2))
    return (input_grad, new_weights, *results)


def solution(mesh):
    split = Mesh(mesh.devices.reshape(2, 4, 8, 2, 2), ALL)
    field = P(None, LAT, LON, None)
    state = P(ALL, None, None)
    return jax.shard_map(
        per_device,
        mesh=split,
        in_specs=(field, field, state, state, state),
        out_specs=(field, P(), state, state, state, state),
        check_vma=False,
    )
```

```python
import math

import jax
import jax.numpy as jnp
from jax import lax
from jax.experimental import pallas as pl
from jax.experimental.pallas import tpu as pltpu
from jax.sharding import Mesh
from jax.sharding import PartitionSpec as P


TAPS = 9
ORDER = (1, 4, 7, 0, 2, 3, 5, 6, 8)
ALL = ("xl", "y", "z", "xh", "c")
LAT = ("xl", "y")
LON = ("z", "xh", "c")
PLANE = ("xl", "y", "xh")
BF16 = jnp.bfloat16
F32 = jnp.float32

learn_rate = 0.01
beta_one = 0.9
beta_two = 0.999
adam_eps = 1e-08
decay_rate = 0.1
step_count = 10.0
norm_eps = 1e-06


def rows_of(shape, dim):
    return lax.broadcasted_iota(jnp.int32, shape, dim)


def channel_of(core, plane, z, k):
    lat, xh = plane // 2, plane % 2
    return (((lat * 8 + z) * 2 + xh) * 2 + core) * 2 + k


def ring_channel(p, core, z):
    arrival, plane, k = p // 32, (p // 2) % 16, p % 2
    step = jnp.where(arrival <= 4, -arrival, arrival - 4)
    return channel_of(core, plane, (z + step + 8) % 8, k)


def row_channel(p):
    plane, z, rest = p // 32, (p // 4) % 8, p % 4
    return channel_of(rest // 2, plane, z, rest % 2)


def neighbours(count, circular):
    forward = [(i, i + 1) for i in range(count - 1)]
    if circular:
        forward.append((count - 1, 0))
    return forward, [(b, a) for a, b in forward]


def row_halo(first, last):
    forward, backward = neighbours(8, False)
    return lax.ppermute(last, LAT, forward), lax.ppermute(first, LAT, backward)


def col_halo(parts, last_col):
    east = jnp.concatenate([part[:, :, last_col : last_col + 1] for part in parts], axis=0)
    west = jnp.concatenate([part[:, :, :1] for part in parts], axis=0)
    forward, backward = neighbours(32, True)
    return lax.ppermute(east, LON, forward), lax.ppermute(west, LON, backward)


def swap(array):
    return lax.ppermute(array, "c", [(0, 1), (1, 0)])


def store_halves(core_ref, lhs, window_of, keep_ref, send_ref):
    half = keep_ref.shape[1]
    own = pl.multiple_of(core_ref[0] * half, half)
    other = pl.multiple_of((1 - core_ref[0]) * half, half)
    send_ref[...] = window_of(lhs, pl.ds(other, half)).astype(BF16)
    keep_ref[...] = window_of(lhs, pl.ds(own, half))


def centre_kernel(core_ref, lhs_ref, above_ref, rows_ref, below_ref, keep_ref, send_ref):
    block = above_ref.shape[0]
    row = pl.program_id(0)

    def dots(pieces, outs):
        total = None
        for start, ref, first, count in pieces:
            part = jnp.dot(
                lhs_ref[:, start : start + count],
                ref[first : first + count, outs],
                preferred_element_type=F32,
            )
            total = part if total is None else total + part
        return total

    plans = (
        ((0, rows_ref, block, 3 * block), (3 * block, below_ref, 0, block)),
        ((0, rows_ref, 0, 4 * block),),
        ((0, above_ref, 0, block), (block, rows_ref, 0, 3 * block)),
    )
    for index, plan in enumerate(plans):

        @pl.when(row == index)
        def _(plan=plan):
            store_halves(core_ref, None, lambda _, outs: dots(plan, outs), keep_ref, send_ref)


def centre_grads(core, lhs, above, rows, below):
    chans, outs = lhs.shape[0], rows.shape[1]
    half = outs // 2
    whole = lambda array: pl.BlockSpec(array.shape, lambda t: (0,) * array.ndim)
    return pl.pallas_call(
        centre_kernel,
        grid=(3,),
        in_specs=[
            pl.BlockSpec(memory_space=pltpu.SMEM),
            whole(lhs),
            whole(above),
            whole(rows),
            whole(below),
        ],
        out_specs=[pl.BlockSpec((chans, half), lambda t: (0, t))] * 2,
        out_shape=[
            jax.ShapeDtypeStruct((chans, 3 * half), F32),
            jax.ShapeDtypeStruct((chans, 3 * half), BF16),
        ],
        compiler_params=pltpu.CompilerParams(vmem_limit_bytes=48 * 1024 * 1024),
        cost_estimate=pl.CostEstimate(
            flops=2 * chans * lhs.shape[1] * 3 * outs, bytes_accessed=8_000_000, transcendentals=0
        ),
        name="centre_grads",
    )(core, lhs, above, rows, below)


def side_kernel(
    core_ref, lhs_ref, above_ref, rows_ref, below_ref, left_ref, right_ref,
    field_ref, keep_ref, send_ref, *, cols, padded_cols,
):
    step = pl.program_id(0)
    block = above_ref.shape[0]
    batch = block // padded_cols

    @pl.when(step == 0)
    def _():
        index = lax.broadcasted_iota(jnp.int32, (padded_cols, 1), 0)
        for line in range(6 * batch):
            first = line * padded_cols
            if line < batch:
                ref, start = above_ref, first
            elif line < 5 * batch:
                ref, start = rows_ref, first - block
            else:
                ref, start = below_ref, first - 5 * block
            centre = ref[start : start + padded_cols, :]
            field_ref[1, first : first + padded_cols, :] = centre
            wide = centre.astype(F32)
            east = pltpu.roll(wide, padded_cols - 1, 0)
            east = jnp.where(index == cols - 1, right_ref[line // batch, line % batch].astype(F32), east)
            field_ref[0, first : first + padded_cols, :] = east.astype(BF16)
            west = pltpu.roll(wide, 1, 0)
            west = jnp.where(index == 0, left_ref[line // batch, line % batch].astype(F32), west)
            field_ref[2, first : first + padded_cols, :] = west.astype(BF16)

    row, side = step // 2, 2 * (step % 2)
    start = pl.multiple_of((2 - row) * block, block)

    def window_dot(_, outs):
        return jnp.dot(
            lhs_ref[...],
            field_ref[side, pl.ds(start, 4 * block), outs],
            preferred_element_type=F32,
        )

    store_halves(core_ref, None, window_dot, keep_ref, send_ref)


def side_grads(core, lhs, above, rows, below, left, right, cols, padded_cols):
    chans, outs = lhs.shape[0], rows.shape[1]
    half = outs // 2
    whole = lambda array: pl.BlockSpec(array.shape, lambda t: (0,) * array.ndim)
    length = rows.shape[0] * 3 // 2
    return pl.pallas_call(
        lambda *refs: side_kernel(*refs, cols=cols, padded_cols=padded_cols),
        grid=(6,),
        in_specs=[pl.BlockSpec(memory_space=pltpu.SMEM)]
        + [whole(array) for array in (lhs, above, rows, below, left, right)],
        out_specs=[pl.BlockSpec((3, length, outs), lambda t: (0, 0, 0))]
        + [pl.BlockSpec((chans, half), lambda t: (0, t))] * 2,
        out_shape=[
            jax.ShapeDtypeStruct((3, length, outs), BF16),
            jax.ShapeDtypeStruct((chans, 6 * half), F32),
            jax.ShapeDtypeStruct((chans, 6 * half), BF16),
        ],
        compiler_params=pltpu.CompilerParams(vmem_limit_bytes=56 * 1024 * 1024),
        cost_estimate=pl.CostEstimate(
            flops=2 * chans * lhs.shape[1] * 6 * outs, bytes_accessed=16_000_000, transcendentals=0
        ),
        name="side_grads",
    )(core, lhs, above, rows, below, left, right)


def pull_kernel(
    field_ref, own_ref, other_ref, own_order_ref, other_order_ref, out_ref, *, block
):
    step = pl.program_id(0)
    outs = field_ref.shape[2]
    result = None
    for weight_ref, order_ref in ((own_ref, own_order_ref), (other_ref, other_order_ref)):
        total = jnp.zeros((block, weight_ref.shape[0]), F32)
        for tap in range(TAPS):
            row, col = divmod(tap, 3)
            start = pl.multiple_of((step + 2 - row) * block, block)
            total = total + lax.dot_general(
                field_ref[col, pl.ds(start, block), :],
                weight_ref[:, tap * outs : (tap + 1) * outs],
                (((1,), (1,)), ((), ())),
                preferred_element_type=F32,
            )
        part = jnp.dot(total.astype(BF16), order_ref[...], preferred_element_type=F32)
        result = part if result is None else result + part
    out_ref[...] = result.astype(BF16)


def pulled(fields, own, other, own_order, other_order):
    block = fields.shape[1] // 6
    chans = own_order.shape[1]
    operands = (fields, own, other, own_order, other_order)
    whole = lambda array: pl.BlockSpec(array.shape, lambda i: (0,) * array.ndim)
    return pl.pallas_call(
        lambda *refs: pull_kernel(*refs, block=block),
        grid=(4,),
        in_specs=[whole(array) for array in operands],
        out_specs=pl.BlockSpec((block, chans), lambda i: (i, 0)),
        out_shape=jax.ShapeDtypeStruct((4 * block, chans), BF16),
        compiler_params=pltpu.CompilerParams(vmem_limit_bytes=48 * 1024 * 1024),
        cost_estimate=pl.CostEstimate(
            flops=2 * 4 * block * chans * own.shape[1],
            bytes_accessed=14_000_000,
            transcendentals=0,
        ),
        name="pulled",
    )(*operands)


def clip_factor(square_sum, max_norm):
    return jnp.minimum(1.0, max_norm / (jnp.sqrt(square_sum) + norm_eps))


def adam(clip, grad, master, moment_one, moment_two):
    clipped = clip * grad
    new_one = beta_one * moment_one + (1.0 - beta_one) * clipped
    new_two = beta_two * moment_two + (1.0 - beta_two) * clipped * clipped
    first_hat = new_one / (1.0 - beta_one**step_count)
    second_hat = new_two / (1.0 - beta_two**step_count)
    new_master = master - learn_rate * (
        first_hat / (jnp.sqrt(second_hat) + adam_eps) + decay_rate * master
    )
    return new_master, new_one, new_two, clipped


def join_kernel(core_ref, order_ref, own_ref, other_ref, out_ref):
    half = own_ref.shape[1] // TAPS
    own = pl.multiple_of(core_ref[0] * half, half)
    other = pl.multiple_of((1 - core_ref[0]) * half, half)
    for lane, ref in ((own, own_ref), (other, other_ref)):
        rows = jnp.dot(order_ref[...], ref[...], preferred_element_type=F32).astype(BF16)
        for index, tap in enumerate(ORDER):
            out_ref[tap, :, pl.ds(lane, half)] = rows[:, index * half : (index + 1) * half]


def joined(core, order, own, other):
    chans, wide = own.shape
    half = wide // TAPS
    block = order.shape[0]
    return pl.pallas_call(
        join_kernel,
        grid=(chans // block,),
        in_specs=[
            pl.BlockSpec(memory_space=pltpu.SMEM),
            pl.BlockSpec(order.shape, lambda i: (0, 0)),
            pl.BlockSpec((block, wide), lambda i: (i, 0)),
            pl.BlockSpec((block, wide), lambda i: (i, 0)),
        ],
        out_specs=pl.BlockSpec((TAPS, block, 2 * half), lambda i: (0, i, 0)),
        out_shape=jax.ShapeDtypeStruct((TAPS, chans, 2 * half), BF16),
        name="joined",
    )(core, order, own, other)


def around_ring(chunk, after):
    chunk, _ = lax.optimization_barrier((chunk, after))
    up = [(i, (i + 1) % 8) for i in range(8)]
    down = [(i, (i - 1) % 8) for i in range(8)]
    below, above = [chunk], [chunk]
    for _ in range(4):
        below.append(lax.ppermute(below[-1], "z", up))
    for _ in range(3):
        above.append(lax.ppermute(above[-1], "z", down))
    return jnp.concatenate(below + above[1:], axis=0)


def to_all(piece, axes, count):
    copies = jnp.broadcast_to(piece[None], (count, *piece.shape))
    return lax.all_to_all(copies, axes, 0, 0, tiled=True)


def halves(array, core):
    half = array.shape[-1] // 2
    low, high = array[..., :half], array[..., half:]
    return jnp.where(core == 0, low, high), jnp.where(core == 0, high, low)


def in_core_order(own, other, core, axis):
    return jnp.where(
        core == 0,
        jnp.concatenate([own, other], axis=axis),
        jnp.concatenate([other, own], axis=axis),
    )


def per_device(activations, upstream, master, moment_one, moment_two):
    batch, lat_rows, lon_cols, chans = activations.shape
    outs = upstream.shape[3]
    half = outs // 2
    wide = TAPS * half
    padded_cols = -(-lon_cols // 32) * 32
    extra = padded_cols - lon_cols
    core = lax.axis_index("c")
    core_ref = core.reshape(1).astype(jnp.int32)
    square = (chans, chans)

    def padded(field):
        return jnp.pad(
            jnp.transpose(field, (1, 0, 2, 3)), ((0, 0), (0, 0), (0, extra), (0, 0))
        )

    def flat(rows):
        return rows.reshape(-1, rows.shape[3])

    above, below = row_halo(padded(upstream[:, :1]), padded(upstream[:, -1:]))
    up_rows = padded(upstream)
    order = (row_channel(rows_of(square, 0)) == rows_of(square, 1)).astype(BF16)
    lhs = lax.dot_general(
        order, flat(padded(activations)), (((1,), (1,)), ((), ())), preferred_element_type=F32
    ).astype(BF16)
    state = jnp.stack([master, moment_one, moment_two])
    own_state, other_state = halves(state, core)
    other_state = swap(other_state)
    state = in_core_order(own_state, other_state, core, 1)
    state = jnp.stack([state[:, :, tap] for tap in ORDER], axis=2).reshape(12, wide)
    left, right = col_halo((above, up_rows, below), lon_cols - 1)
    pieces = (flat(above), flat(up_rows), flat(below))
    old_piece = master.astype(BF16).reshape(2, TAPS * outs)
    old_plane = to_all(old_piece, PLANE, 16).reshape(32, TAPS * outs)
    keep_one, send_one = centre_grads(core_ref, lhs, *pieces)
    swapped_one = swap(send_one)
    left, right, keep_one = lax.optimization_barrier((left, right, keep_one))
    fields, keep_two, send_two = side_grads(
        core_ref, lhs, *pieces, left, right, lon_cols, padded_cols
    )
    swapped_two = swap(send_two)
    pair_sum = jnp.concatenate(
        [
            (keep_one + swapped_one.astype(F32)).astype(BF16),
            (keep_two + swapped_two.astype(F32)).astype(BF16),
        ],
        axis=1,
    ).reshape(16, 32, wide)
    parts = lax.all_to_all(pair_sum, PLANE, 0, 0, tiled=True)
    old_own = around_ring(old_plane, pair_sum)
    plane_sum = jnp.sum(parts.astype(F32), axis=0).astype(BF16).reshape(8, 4, wide)
    parts = lax.all_to_all(plane_sum, ("z",), 0, 0, tiled=True)
    grad = jnp.sum(parts.astype(F32), axis=0)

    square_sum = jnp.sum(to_all(jnp.sum(grad * grad).reshape(1, 1), ALL, 256)).reshape(1, 1)
    clip = clip_factor(square_sum, math.sqrt(float(chans * TAPS * outs)))
    results = jnp.stack(adam(clip, grad, *state.reshape(3, 4, wide)))
    new_line = to_all(results[0].astype(BF16), ("z",), 8).reshape(32, wide)
    own = to_all(new_line, PLANE, 16).reshape(chans, wide)

    results = results.reshape(4, 4, TAPS, half)
    results = jnp.stack([results[:, :, ORDER.index(tap)] for tap in range(TAPS)], axis=2)
    mine = jnp.where(core == 0, results[:, :2], results[:, 2:])
    theirs = jnp.where(core == 0, results[:, 2:], results[:, :2])
    results = in_core_order(mine, swap(theirs), core, 3)

    old_other = swap(old_own)
    fields, old_own, old_other, _ = lax.optimization_barrier(
        (fields, old_own, old_other, new_line)
    )
    z = lax.axis_index("z")
    across = (chans // 2, chans)
    old_orders = [
        (ring_channel(rows_of(across, 0), which, z) == rows_of(across, 1)).astype(BF16)
        for which in (core, 1 - core)
    ]
    pulled_rows = pulled(fields, old_own, old_other, *old_orders)
    input_grad = pulled_rows.reshape(lat_rows, batch, padded_cols, chans)
    input_grad = jnp.transpose(input_grad[:, :, :lon_cols], (1, 0, 2, 3))

    lat_block = (chans // 4, chans // 4)
    back = (rows_of(lat_block, 0) == row_channel(rows_of(lat_block, 1))).astype(BF16)
    new_weights = jnp.transpose(joined(core_ref, back, own, swap(own)), (1, 0, 2))
    return (input_grad, new_weights, *results)


def solution(mesh):
    split = Mesh(mesh.devices.reshape(2, 4, 8, 2, 2), ALL)
    field = P(None, LAT, LON, None)
    state = P(ALL, None, None)
    return jax.shard_map(
        per_device,
        mesh=split,
        in_specs=(field, field, state, state, state),
        out_specs=(field, P(), state, state, state, state),
        check_vma=False,
    )
```

```python
import math

import jax
import jax.numpy as jnp
import numpy as np
from jax import lax
from jax.experimental import pallas as pl
from jax.experimental.pallas import tpu as pltpu
from jax.sharding import Mesh
from jax.sharding import PartitionSpec as P


TAPS = 9
ORDER = (1, 4, 7, 0, 2, 3, 5, 6, 8)
ALL = ("xl", "y", "z", "xh", "c")
LAT = ("xl", "y")
LON = ("z", "xh", "c")
PLANE = ("xl", "y", "xh")
BF16 = jnp.bfloat16
F32 = jnp.float32

learn_rate = 0.01
beta_one = 0.9
beta_two = 0.999
adam_eps = 1e-08
decay_rate = 0.1
step_count = 10.0
norm_eps = 1e-06


def rows_of(shape, dim):
    return lax.broadcasted_iota(jnp.int32, shape, dim)


def channel_of(core, plane, z, k):
    lat, xh = plane // 2, plane % 2
    return (((lat * 8 + z) * 2 + xh) * 2 + core) * 2 + k


def ring_channel(p, core, z):
    arrival, plane, k = p // 32, (p // 2) % 16, p % 2
    step = jnp.where(arrival <= 4, -arrival, arrival - 4)
    return channel_of(core, plane, (z + step + 8) % 8, k)


def row_channel(p):
    plane, z, rest = p // 32, (p // 4) % 8, p % 4
    return channel_of(rest // 2, plane, z, rest % 2)


def neighbours(count, circular):
    forward = [(i, i + 1) for i in range(count - 1)]
    if circular:
        forward.append((count - 1, 0))
    return forward, [(b, a) for a, b in forward]


def row_halo(first, last):
    forward, backward = neighbours(8, False)
    return lax.ppermute(last, LAT, forward), lax.ppermute(first, LAT, backward)


def col_halo(parts, last_col):
    east = jnp.concatenate([part[:, :, last_col : last_col + 1] for part in parts], axis=0)
    west = jnp.concatenate([part[:, :, :1] for part in parts], axis=0)
    forward, backward = neighbours(32, True)
    return lax.ppermute(east, LON, forward), lax.ppermute(west, LON, backward)


def swap(array):
    return lax.ppermute(array, "c", [(0, 1), (1, 0)])


def store_halves(core_ref, lhs, window_of, keep_ref, send_ref):
    half = keep_ref.shape[1]
    own = pl.multiple_of(core_ref[0] * half, half)
    other = pl.multiple_of((1 - core_ref[0]) * half, half)
    send_ref[...] = window_of(lhs, pl.ds(other, half)).astype(BF16)
    keep_ref[...] = window_of(lhs, pl.ds(own, half))


def centre_kernel(core_ref, lhs_ref, above_ref, rows_ref, below_ref, keep_ref, send_ref):
    block = above_ref.shape[0]
    row = pl.program_id(0)

    def dots(pieces, outs):
        total = None
        for start, ref, first, count in pieces:
            part = jnp.dot(
                lhs_ref[:, start : start + count],
                ref[first : first + count, outs],
                preferred_element_type=F32,
            )
            total = part if total is None else total + part
        return total

    plans = (
        ((0, rows_ref, block, 3 * block), (3 * block, below_ref, 0, block)),
        ((0, rows_ref, 0, 4 * block),),
        ((0, above_ref, 0, block), (block, rows_ref, 0, 3 * block)),
    )
    for index, plan in enumerate(plans):

        @pl.when(row == index)
        def _(plan=plan):
            store_halves(core_ref, None, lambda _, outs: dots(plan, outs), keep_ref, send_ref)


def centre_grads(core, lhs, above, rows, below):
    chans, outs = lhs.shape[0], rows.shape[1]
    half = outs // 2
    whole = lambda array: pl.BlockSpec(array.shape, lambda t: (0,) * array.ndim)
    return pl.pallas_call(
        centre_kernel,
        grid=(3,),
        in_specs=[
            pl.BlockSpec(memory_space=pltpu.SMEM),
            whole(lhs),
            whole(above),
            whole(rows),
            whole(below),
        ],
        out_specs=[pl.BlockSpec((chans, half), lambda t: (0, t))] * 2,
        out_shape=[
            jax.ShapeDtypeStruct((chans, 3 * half), F32),
            jax.ShapeDtypeStruct((chans, 3 * half), BF16),
        ],
        compiler_params=pltpu.CompilerParams(vmem_limit_bytes=48 * 1024 * 1024),
        cost_estimate=pl.CostEstimate(
            flops=2 * chans * lhs.shape[1] * 3 * outs, bytes_accessed=8_000_000, transcendentals=0
        ),
        name="centre_grads",
    )(core, lhs, above, rows, below)


def side_kernel(
    core_ref, lhs_ref, above_ref, rows_ref, below_ref, left_ref, right_ref,
    field_ref, keep_ref, send_ref, *, cols, padded_cols,
):
    step = pl.program_id(0)
    block = above_ref.shape[0]
    batch = block // padded_cols

    @pl.when(step == 0)
    def _():
        index = lax.broadcasted_iota(jnp.int32, (padded_cols, 1), 0)
        for line in range(6 * batch):
            first = line * padded_cols
            if line < batch:
                ref, start = above_ref, first
            elif line < 5 * batch:
                ref, start = rows_ref, first - block
            else:
                ref, start = below_ref, first - 5 * block
            centre = ref[start : start + padded_cols, :]
            field_ref[1, first : first + padded_cols, :] = centre
            wide = centre.astype(F32)
            east = pltpu.roll(wide, padded_cols - 1, 0)
            east = jnp.where(index == cols - 1, right_ref[line // batch, line % batch].astype(F32), east)
            field_ref[0, first : first + padded_cols, :] = east.astype(BF16)
            west = pltpu.roll(wide, 1, 0)
            west = jnp.where(index == 0, left_ref[line // batch, line % batch].astype(F32), west)
            field_ref[2, first : first + padded_cols, :] = west.astype(BF16)

    row, side = step // 2, 2 * (step % 2)
    start = pl.multiple_of((2 - row) * block, block)

    def window_dot(_, outs):
        return jnp.dot(
            lhs_ref[...],
            field_ref[side, pl.ds(start, 4 * block), outs],
            preferred_element_type=F32,
        )

    store_halves(core_ref, None, window_dot, keep_ref, send_ref)


def side_grads(core, lhs, above, rows, below, left, right, cols, padded_cols):
    chans, outs = lhs.shape[0], rows.shape[1]
    half = outs // 2
    whole = lambda array: pl.BlockSpec(array.shape, lambda t: (0,) * array.ndim)
    length = rows.shape[0] * 3 // 2
    return pl.pallas_call(
        lambda *refs: side_kernel(*refs, cols=cols, padded_cols=padded_cols),
        grid=(6,),
        in_specs=[pl.BlockSpec(memory_space=pltpu.SMEM)]
        + [whole(array) for array in (lhs, above, rows, below, left, right)],
        out_specs=[pl.BlockSpec((3, length, outs), lambda t: (0, 0, 0))]
        + [pl.BlockSpec((chans, half), lambda t: (0, t))] * 2,
        out_shape=[
            jax.ShapeDtypeStruct((3, length, outs), BF16),
            jax.ShapeDtypeStruct((chans, 6 * half), F32),
            jax.ShapeDtypeStruct((chans, 6 * half), BF16),
        ],
        compiler_params=pltpu.CompilerParams(vmem_limit_bytes=56 * 1024 * 1024),
        cost_estimate=pl.CostEstimate(
            flops=2 * chans * lhs.shape[1] * 6 * outs, bytes_accessed=16_000_000, transcendentals=0
        ),
        name="side_grads",
    )(core, lhs, above, rows, below, left, right)


def pull_kernel(
    field_ref, own_ref, other_ref, own_order_ref, other_order_ref, out_ref, *, block
):
    step = pl.program_id(0)
    outs = field_ref.shape[2]
    result = None
    for weight_ref, order_ref in ((own_ref, own_order_ref), (other_ref, other_order_ref)):
        total = jnp.zeros((block, weight_ref.shape[0]), F32)
        for tap in range(TAPS):
            row, col = divmod(tap, 3)
            start = pl.multiple_of((step + 2 - row) * block, block)
            total = total + lax.dot_general(
                field_ref[col, pl.ds(start, block), :],
                weight_ref[:, tap * outs : (tap + 1) * outs],
                (((1,), (1,)), ((), ())),
                preferred_element_type=F32,
            )
        part = jnp.dot(total.astype(BF16), order_ref[...], preferred_element_type=F32)
        result = part if result is None else result + part
    out_ref[...] = result.astype(BF16)


def pulled(fields, own, other, own_order, other_order):
    block = fields.shape[1] // 6
    chans = own_order.shape[1]
    operands = (fields, own, other, own_order, other_order)
    whole = lambda array: pl.BlockSpec(array.shape, lambda i: (0,) * array.ndim)
    return pl.pallas_call(
        lambda *refs: pull_kernel(*refs, block=block),
        grid=(4,),
        in_specs=[whole(array) for array in operands],
        out_specs=pl.BlockSpec((block, chans), lambda i: (i, 0)),
        out_shape=jax.ShapeDtypeStruct((4 * block, chans), BF16),
        compiler_params=pltpu.CompilerParams(vmem_limit_bytes=48 * 1024 * 1024),
        cost_estimate=pl.CostEstimate(
            flops=2 * 4 * block * chans * own.shape[1],
            bytes_accessed=14_000_000,
            transcendentals=0,
        ),
        name="pulled",
    )(*operands)


def clip_factor(square_sum, max_norm):
    return jnp.minimum(1.0, max_norm / (jnp.sqrt(square_sum) + norm_eps))


def adam(clip, grad, master, moment_one, moment_two):
    clipped = clip * grad
    new_one = beta_one * moment_one + (1.0 - beta_one) * clipped
    new_two = beta_two * moment_two + (1.0 - beta_two) * clipped * clipped
    first_hat = new_one / (1.0 - beta_one**step_count)
    second_hat = new_two / (1.0 - beta_two**step_count)
    new_master = master - learn_rate * (
        first_hat / (jnp.sqrt(second_hat) + adam_eps) + decay_rate * master
    )
    return new_master, new_one, new_two, clipped


def join_kernel(_, order_ref, part_ref, *refs):
    out_ref = refs[-1]
    half = out_ref.shape[2]
    rows = jnp.dot(order_ref[...], part_ref[...], preferred_element_type=F32).astype(BF16)
    for index, tap in enumerate(ORDER):
        out_ref[tap] = rows[:, index * half : (index + 1) * half]


def joined(lane, order, part, out):
    chans, wide = part.shape
    half = wide // TAPS
    block = order.shape[0]
    operands = (order, part) if out is None else (order, part, out)
    return pl.pallas_call(
        join_kernel,
        grid_spec=pltpu.PrefetchScalarGridSpec(
            num_scalar_prefetch=1,
            grid=(chans // block,),
            in_specs=[
                pl.BlockSpec(order.shape, lambda i, lane_ref: (0, 0)),
                pl.BlockSpec((block, wide), lambda i, lane_ref: (i, 0)),
                pl.BlockSpec(memory_space=pl.ANY),
            ][: len(operands)],
            out_specs=pl.BlockSpec((TAPS, block, half), lambda i, lane_ref: (0, i, lane_ref[0])),
        ),
        out_shape=jax.ShapeDtypeStruct((TAPS, chans, 2 * half), BF16),
        input_output_aliases={} if out is None else {3: 0},
        cost_estimate=pl.CostEstimate(
            flops=2 * part.size * block, bytes_accessed=8 * part.size, transcendentals=0
        ),
        name="joined",
    )(lane, *operands)


def around_ring(chunk, early, late):
    up = [(i, (i + 1) % 8) for i in range(8)]
    down = [(i, (i - 1) % 8) for i in range(8)]
    chunk, _ = lax.optimization_barrier((chunk, early))
    first = lax.ppermute(chunk, "z", up), lax.ppermute(chunk, "z", down)
    first, _ = lax.optimization_barrier((first, late))
    below, above = [chunk, first[0]], [first[1]]
    for _ in range(3):
        below.append(lax.ppermute(below[-1], "z", up))
    for _ in range(2):
        above.append(lax.ppermute(above[-1], "z", down))
    return jnp.concatenate(below + above, axis=0)


def to_all(piece, axes, count):
    copies = jnp.broadcast_to(piece[None], (count, *piece.shape))
    return lax.all_to_all(copies, axes, 0, 0, tiled=True)


def halves(array, core):
    half = array.shape[-1] // 2
    low, high = array[..., :half], array[..., half:]
    return jnp.where(core == 0, low, high), jnp.where(core == 0, high, low)


def in_core_order(own, other, core, axis):
    return jnp.where(
        core == 0,
        jnp.concatenate([own, other], axis=axis),
        jnp.concatenate([other, own], axis=axis),
    )


def per_device(activations, upstream, master, moment_one, moment_two):
    batch, lat_rows, lon_cols, chans = activations.shape
    outs = upstream.shape[3]
    half = outs // 2
    wide = TAPS * half
    padded_cols = -(-lon_cols // 32) * 32
    extra = padded_cols - lon_cols
    core = lax.axis_index("c")
    core_ref = core.reshape(1).astype(jnp.int32)

    def padded(field):
        return jnp.pad(
            jnp.transpose(field, (1, 0, 2, 3)), ((0, 0), (0, 0), (0, extra), (0, 0))
        )

    def flat(rows):
        return rows.reshape(-1, rows.shape[3])

    above, below = row_halo(padded(upstream[:, :1]), padded(upstream[:, -1:]))
    up_rows = padded(upstream)
    rows = np.arange(chans)
    order = jnp.asarray(row_channel(rows)[:, None] == rows[None, :], BF16)
    lhs = lax.dot_general(
        order, flat(padded(activations)), (((1,), (1,)), ((), ())), preferred_element_type=F32
    ).astype(BF16)
    left, right = col_halo((above, up_rows, below), lon_cols - 1)
    pieces = (flat(above), flat(up_rows), flat(below))
    old_piece = master.astype(BF16).reshape(2, TAPS * outs)
    old_plane = to_all(old_piece, PLANE, 16).reshape(32, TAPS * outs)
    keep_one, send_one = centre_grads(core_ref, lhs, *pieces)
    swapped_one = swap(send_one)
    left, right, keep_one = lax.optimization_barrier((left, right, keep_one))
    fields, keep_two, send_two = side_grads(
        core_ref, lhs, *pieces, left, right, lon_cols, padded_cols
    )
    swapped_two = swap(send_two)
    pair_sum = jnp.concatenate(
        [
            (keep_one + swapped_one.astype(F32)).astype(BF16),
            (keep_two + swapped_two.astype(F32)).astype(BF16),
        ],
        axis=1,
    ).reshape(16, 32, wide)
    state = jnp.stack([master, moment_one, moment_two])
    state, pair_sum = lax.optimization_barrier((state, pair_sum))
    own_state, other_state = halves(state, core)
    other_state = swap(other_state)
    state = in_core_order(own_state, other_state, core, 1)
    state = jnp.stack([state[:, :, tap] for tap in ORDER], axis=2).reshape(12, wide)
    parts = lax.all_to_all(pair_sum, PLANE, 0, 0, tiled=True)
    old_own = around_ring(old_plane, keep_one, pair_sum)
    plane_sum = jnp.sum(parts.astype(F32), axis=0).astype(BF16).reshape(8, 4, wide)
    parts = lax.all_to_all(plane_sum, ("z",), 0, 0, tiled=True)
    grad = jnp.sum(parts.astype(F32), axis=0)

    square_sum = jnp.sum(to_all(jnp.sum(grad * grad).reshape(1, 1), ALL, 256)).reshape(1, 1)
    clip = clip_factor(square_sum, math.sqrt(float(chans * TAPS * outs)))
    results = jnp.stack(adam(clip, grad, *state.reshape(3, 4, wide)))
    new_line = to_all(results[0].astype(BF16), ("z",), 8).reshape(32, wide)
    own = to_all(new_line, PLANE, 16).reshape(chans, wide)

    results = results.reshape(4, 4, TAPS, half)
    results = jnp.stack([results[:, :, ORDER.index(tap)] for tap in range(TAPS)], axis=1)
    mine = jnp.where(core == 0, results[:, :, :2], results[:, :, 2:])
    theirs = jnp.where(core == 0, results[:, :, 2:], results[:, :, :2])
    results = in_core_order(mine, swap(theirs), core, 3)
    results = [jnp.transpose(result, (1, 0, 2)) for result in results]

    old_other = swap(old_own)
    fields, old_own, old_other, _ = lax.optimization_barrier(
        (fields, old_own, old_other, new_line)
    )
    z = lax.axis_index("z")
    across = (chans // 2, chans)
    old_orders = [
        (ring_channel(rows_of(across, 0), which, z) == rows_of(across, 1)).astype(BF16)
        for which in (core, 1 - core)
    ]
    pulled_rows = pulled(fields, old_own, old_other, *old_orders)
    input_grad = pulled_rows.reshape(lat_rows, batch, padded_cols, chans)
    input_grad = jnp.transpose(input_grad[:, :, :lon_cols], (1, 0, 2, 3))

    rows = np.arange(chans // 4)
    back = jnp.asarray(rows[:, None] == row_channel(rows)[None, :], BF16)
    other = swap(own)
    out = joined(core_ref, back, own, None)
    out = joined(1 - core_ref, back, other, out)
    new_weights = jnp.transpose(out, (1, 0, 2))
    return (input_grad, new_weights, *results)


def solution(mesh):
    split = Mesh(mesh.devices.reshape(2, 4, 8, 2, 2), ALL)
    field = P(None, LAT, LON, None)
    state = P(ALL, None, None)
    return jax.shard_map(
        per_device,
        mesh=split,
        in_specs=(field, field, state, state, state),
        out_specs=(field, P(), state, state, state, state),
        check_vma=False,
    )
```

```python
import math

import jax
import jax.numpy as jnp
import numpy as np
from jax import lax
from jax.experimental import pallas as pl
from jax.experimental.pallas import tpu as pltpu
from jax.sharding import Mesh
from jax.sharding import PartitionSpec as P


TAPS = 9
ORDER = (1, 4, 7, 0, 2, 3, 5, 6, 8)
ALL = ("xl", "y", "z", "xh", "c")
LAT = ("xl", "y")
LON = ("z", "xh", "c")
PLANE = ("xl", "y", "xh")
BF16 = jnp.bfloat16
F32 = jnp.float32

learn_rate = 0.01
beta_one = 0.9
beta_two = 0.999
adam_eps = 1e-08
decay_rate = 0.1
step_count = 10.0
norm_eps = 1e-06


def rows_of(shape, dim):
    return lax.broadcasted_iota(jnp.int32, shape, dim)


def channel_of(core, plane, z, k):
    lat, xh = plane // 2, plane % 2
    return (((lat * 8 + z) * 2 + xh) * 2 + core) * 2 + k


def ring_channel(p, core, z):
    arrival, plane, k = p // 32, (p // 2) % 16, p % 2
    step = jnp.where(arrival <= 4, -arrival, arrival - 4)
    return channel_of(core, plane, (z + step + 8) % 8, k)


def row_channel(p):
    plane, z, rest = p // 32, (p // 4) % 8, p % 4
    return channel_of(rest // 2, plane, z, rest % 2)


def neighbours(count, circular):
    forward = [(i, i + 1) for i in range(count - 1)]
    if circular:
        forward.append((count - 1, 0))
    return forward, [(b, a) for a, b in forward]


def row_halo(first, last):
    forward, backward = neighbours(8, False)
    return lax.ppermute(last, LAT, forward), lax.ppermute(first, LAT, backward)


def col_halo(parts, last_col):
    east = jnp.concatenate([part[:, :, last_col : last_col + 1] for part in parts], axis=0)
    west = jnp.concatenate([part[:, :, :1] for part in parts], axis=0)
    forward, backward = neighbours(32, True)
    return lax.ppermute(east, LON, forward), lax.ppermute(west, LON, backward)


def swap(array):
    return lax.ppermute(array, "c", [(0, 1), (1, 0)])


def store_halves(core_ref, lhs, window_of, keep_ref, send_ref):
    half = keep_ref.shape[1]
    own = pl.multiple_of(core_ref[0] * half, half)
    other = pl.multiple_of((1 - core_ref[0]) * half, half)
    send_ref[...] = window_of(lhs, pl.ds(other, half)).astype(BF16)
    keep_ref[...] = window_of(lhs, pl.ds(own, half))


def centre_kernel(core_ref, lhs_ref, above_ref, rows_ref, below_ref, keep_ref, send_ref):
    block = above_ref.shape[0]
    row = pl.program_id(0)

    def dots(pieces, outs):
        total = None
        for start, ref, first, count in pieces:
            part = jnp.dot(
                lhs_ref[:, start : start + count],
                ref[first : first + count, outs],
                preferred_element_type=F32,
            )
            total = part if total is None else total + part
        return total

    plans = (
        ((0, rows_ref, block, 3 * block), (3 * block, below_ref, 0, block)),
        ((0, rows_ref, 0, 4 * block),),
        ((0, above_ref, 0, block), (block, rows_ref, 0, 3 * block)),
    )
    for index, plan in enumerate(plans):

        @pl.when(row == index)
        def _(plan=plan):
            store_halves(core_ref, None, lambda _, outs: dots(plan, outs), keep_ref, send_ref)


def centre_grads(core, lhs, above, rows, below):
    chans, outs = lhs.shape[0], rows.shape[1]
    half = outs // 2
    whole = lambda array: pl.BlockSpec(array.shape, lambda t: (0,) * array.ndim)
    return pl.pallas_call(
        centre_kernel,
        grid=(3,),
        in_specs=[
            pl.BlockSpec(memory_space=pltpu.SMEM),
            whole(lhs),
            whole(above),
            whole(rows),
            whole(below),
        ],
        out_specs=[pl.BlockSpec((chans, half), lambda t: (0, t))] * 2,
        out_shape=[
            jax.ShapeDtypeStruct((chans, 3 * half), F32),
            jax.ShapeDtypeStruct((chans, 3 * half), BF16),
        ],
        compiler_params=pltpu.CompilerParams(vmem_limit_bytes=48 * 1024 * 1024),
        cost_estimate=pl.CostEstimate(
            flops=2 * chans * lhs.shape[1] * 3 * outs, bytes_accessed=8_000_000, transcendentals=0
        ),
        name="centre_grads",
    )(core, lhs, above, rows, below)


def side_kernel(
    core_ref, lhs_ref, above_ref, rows_ref, below_ref, left_ref, right_ref,
    field_ref, keep_ref, send_ref, *, cols, padded_cols,
):
    step = pl.program_id(0)
    block = above_ref.shape[0]
    batch = block // padded_cols

    @pl.when(step == 0)
    def _():
        index = lax.broadcasted_iota(jnp.int32, (padded_cols, 1), 0)
        for line in range(6 * batch):
            first = line * padded_cols
            if line < batch:
                ref, start = above_ref, first
            elif line < 5 * batch:
                ref, start = rows_ref, first - block
            else:
                ref, start = below_ref, first - 5 * block
            centre = ref[start : start + padded_cols, :]
            field_ref[1, first : first + padded_cols, :] = centre
            wide = centre.astype(F32)
            east = pltpu.roll(wide, padded_cols - 1, 0)
            east = jnp.where(index == cols - 1, right_ref[line // batch, line % batch].astype(F32), east)
            field_ref[0, first : first + padded_cols, :] = east.astype(BF16)
            west = pltpu.roll(wide, 1, 0)
            west = jnp.where(index == 0, left_ref[line // batch, line % batch].astype(F32), west)
            field_ref[2, first : first + padded_cols, :] = west.astype(BF16)

    row, side = step // 2, 2 * (step % 2)
    start = pl.multiple_of((2 - row) * block, block)

    def window_dot(_, outs):
        return jnp.dot(
            lhs_ref[...],
            field_ref[side, pl.ds(start, 4 * block), outs],
            preferred_element_type=F32,
        )

    store_halves(core_ref, None, window_dot, keep_ref, send_ref)


def side_grads(core, lhs, above, rows, below, left, right, cols, padded_cols):
    chans, outs = lhs.shape[0], rows.shape[1]
    half = outs // 2
    whole = lambda array: pl.BlockSpec(array.shape, lambda t: (0,) * array.ndim)
    length = rows.shape[0] * 3 // 2
    return pl.pallas_call(
        lambda *refs: side_kernel(*refs, cols=cols, padded_cols=padded_cols),
        grid=(6,),
        in_specs=[pl.BlockSpec(memory_space=pltpu.SMEM)]
        + [whole(array) for array in (lhs, above, rows, below, left, right)],
        out_specs=[pl.BlockSpec((3, length, outs), lambda t: (0, 0, 0))]
        + [pl.BlockSpec((chans, half), lambda t: (0, t))] * 2,
        out_shape=[
            jax.ShapeDtypeStruct((3, length, outs), BF16),
            jax.ShapeDtypeStruct((chans, 6 * half), F32),
            jax.ShapeDtypeStruct((chans, 6 * half), BF16),
        ],
        compiler_params=pltpu.CompilerParams(vmem_limit_bytes=56 * 1024 * 1024),
        cost_estimate=pl.CostEstimate(
            flops=2 * chans * lhs.shape[1] * 6 * outs, bytes_accessed=16_000_000, transcendentals=0
        ),
        name="side_grads",
    )(core, lhs, above, rows, below, left, right)


def pull_kernel(
    field_ref, own_ref, other_ref, own_order_ref, other_order_ref, out_ref, *, block
):
    step = pl.program_id(0)
    outs = field_ref.shape[2]
    result = None
    for weight_ref, order_ref in ((own_ref, own_order_ref), (other_ref, other_order_ref)):
        total = jnp.zeros((block, weight_ref.shape[0]), F32)
        for tap in range(TAPS):
            row, col = divmod(tap, 3)
            start = pl.multiple_of((step + 2 - row) * block, block)
            total = total + lax.dot_general(
                field_ref[col, pl.ds(start, block), :],
                weight_ref[:, tap * outs : (tap + 1) * outs],
                (((1,), (1,)), ((), ())),
                preferred_element_type=F32,
            )
        part = jnp.dot(total.astype(BF16), order_ref[...], preferred_element_type=F32)
        result = part if result is None else result + part
    out_ref[...] = result.astype(BF16)


def pulled(fields, own, other, own_order, other_order):
    block = fields.shape[1] // 6
    chans = own_order.shape[1]
    operands = (fields, own, other, own_order, other_order)
    whole = lambda array: pl.BlockSpec(array.shape, lambda i: (0,) * array.ndim)
    return pl.pallas_call(
        lambda *refs: pull_kernel(*refs, block=block),
        grid=(4,),
        in_specs=[whole(array) for array in operands],
        out_specs=pl.BlockSpec((block, chans), lambda i: (i, 0)),
        out_shape=jax.ShapeDtypeStruct((4 * block, chans), BF16),
        compiler_params=pltpu.CompilerParams(vmem_limit_bytes=48 * 1024 * 1024),
        cost_estimate=pl.CostEstimate(
            flops=2 * 4 * block * chans * own.shape[1],
            bytes_accessed=14_000_000,
            transcendentals=0,
        ),
        name="pulled",
    )(*operands)


def clip_factor(square_sum, max_norm):
    return jnp.minimum(1.0, max_norm / (jnp.sqrt(square_sum) + norm_eps))


def adam(clip, grad, master, moment_one, moment_two):
    clipped = clip * grad
    new_one = beta_one * moment_one + (1.0 - beta_one) * clipped
    new_two = beta_two * moment_two + (1.0 - beta_two) * clipped * clipped
    first_hat = new_one / (1.0 - beta_one**step_count)
    second_hat = new_two / (1.0 - beta_two**step_count)
    new_master = master - learn_rate * (
        first_hat / (jnp.sqrt(second_hat) + adam_eps) + decay_rate * master
    )
    return new_master, new_one, new_two, clipped


def join_kernel(core_ref, order_ref, own_ref, other_ref, *refs):
    out_ref = refs[-1]
    half = own_ref.shape[1] // TAPS
    own = pl.multiple_of(core_ref[0] * half, half)
    other = pl.multiple_of((1 - core_ref[0]) * half, half)
    for lane, ref in ((own, own_ref), (other, other_ref)):
        rows = jnp.dot(order_ref[...], ref[...], preferred_element_type=F32).astype(BF16)
        for index, tap in enumerate(ORDER):
            out_ref[tap, :, pl.ds(lane, half)] = rows[:, index * half : (index + 1) * half]


def joined(core, order, own, other, first, out):
    count, wide = other.shape
    half = wide // TAPS
    block = order.shape[0]
    operands = (core, order, own, other) if out is None else (core, order, own, other, out)
    return pl.pallas_call(
        join_kernel,
        grid=(count // block,),
        in_specs=[
            pl.BlockSpec(memory_space=pltpu.SMEM),
            pl.BlockSpec(order.shape, lambda i: (0, 0)),
            pl.BlockSpec((block, wide), lambda i: (i + first, 0)),
            pl.BlockSpec((block, wide), lambda i: (i, 0)),
            pl.BlockSpec(memory_space=pl.ANY),
        ][: len(operands)],
        out_specs=pl.BlockSpec((TAPS, block, 2 * half), lambda i: (0, i + first, 0)),
        out_shape=jax.ShapeDtypeStruct((TAPS, own.shape[0], 2 * half), BF16),
        input_output_aliases={} if out is None else {4: 0},
        cost_estimate=pl.CostEstimate(
            flops=2 * count * wide * block, bytes_accessed=8 * count * wide, transcendentals=0
        ),
        name="joined",
    )(*operands)


def around_ring(chunk, after):
    chunk, _ = lax.optimization_barrier((chunk, after))
    up = [(i, (i + 1) % 8) for i in range(8)]
    down = [(i, (i - 1) % 8) for i in range(8)]
    below, above = [chunk], [chunk]
    for _ in range(4):
        below.append(lax.ppermute(below[-1], "z", up))
    for _ in range(3):
        above.append(lax.ppermute(above[-1], "z", down))
    return jnp.concatenate(below + above[1:], axis=0)


def to_all(piece, axes, count):
    copies = jnp.broadcast_to(piece[None], (count, *piece.shape))
    return lax.all_to_all(copies, axes, 0, 0, tiled=True)


def halves(array, core):
    half = array.shape[-1] // 2
    low, high = array[..., :half], array[..., half:]
    return jnp.where(core == 0, low, high), jnp.where(core == 0, high, low)


def in_core_order(own, other, core, axis):
    return jnp.where(
        core == 0,
        jnp.concatenate([own, other], axis=axis),
        jnp.concatenate([other, own], axis=axis),
    )


def per_device(activations, upstream, master, moment_one, moment_two):
    batch, lat_rows, lon_cols, chans = activations.shape
    outs = upstream.shape[3]
    half = outs // 2
    wide = TAPS * half
    padded_cols = -(-lon_cols // 32) * 32
    extra = padded_cols - lon_cols
    core = lax.axis_index("c")
    core_ref = core.reshape(1).astype(jnp.int32)

    def padded(field):
        return jnp.pad(
            jnp.transpose(field, (1, 0, 2, 3)), ((0, 0), (0, 0), (0, extra), (0, 0))
        )

    def flat(rows):
        return rows.reshape(-1, rows.shape[3])

    above, below = row_halo(padded(upstream[:, :1]), padded(upstream[:, -1:]))
    up_rows = padded(upstream)
    rows = np.arange(chans)
    order = jnp.asarray(row_channel(rows)[:, None] == rows[None, :], BF16)
    lhs = lax.dot_general(
        order, flat(padded(activations)), (((1,), (1,)), ((), ())), preferred_element_type=F32
    ).astype(BF16)
    left, right = col_halo((above, up_rows, below), lon_cols - 1)
    pieces = (flat(above), flat(up_rows), flat(below))
    old_piece = master.astype(BF16).reshape(2, TAPS * outs)
    old_plane = to_all(old_piece, PLANE, 16).reshape(32, TAPS * outs)
    keep_one, send_one = centre_grads(core_ref, lhs, *pieces)
    swapped_one = swap(send_one)
    left, right, keep_one = lax.optimization_barrier((left, right, keep_one))
    fields, keep_two, send_two = side_grads(
        core_ref, lhs, *pieces, left, right, lon_cols, padded_cols
    )
    swapped_two = swap(send_two)
    pair_sum = jnp.concatenate(
        [
            (keep_one + swapped_one.astype(F32)).astype(BF16),
            (keep_two + swapped_two.astype(F32)).astype(BF16),
        ],
        axis=1,
    ).reshape(16, 32, wide)
    *state, pair_sum = lax.optimization_barrier((master, moment_one, moment_two, pair_sum))
    state = jnp.stack(state)
    own_state, other_state = halves(state, core)
    other_state = swap(other_state)
    state = in_core_order(own_state, other_state, core, 1)
    state = jnp.stack([state[:, :, tap] for tap in ORDER], axis=2).reshape(12, wide)
    parts = lax.all_to_all(pair_sum, PLANE, 0, 0, tiled=True)
    old_own = around_ring(old_plane, pair_sum)
    plane_sum = jnp.sum(parts.astype(F32), axis=0).astype(BF16).reshape(8, 4, wide)
    parts = lax.all_to_all(plane_sum, ("z",), 0, 0, tiled=True)
    grad = jnp.sum(parts.astype(F32), axis=0)

    square_sum = jnp.sum(to_all(jnp.sum(grad * grad).reshape(1, 1), ALL, 256)).reshape(1, 1)
    clip = clip_factor(square_sum, math.sqrt(float(chans * TAPS * outs)))
    results = jnp.stack(adam(clip, grad, *state.reshape(3, 4, wide)))
    new_line = to_all(results[0].astype(BF16), ("z",), 8).reshape(32, wide)
    own = to_all(new_line, PLANE, 16).reshape(chans, wide)

    results = results.reshape(4, 4, TAPS, half)
    results = jnp.stack([results[:, :, ORDER.index(tap)] for tap in range(TAPS)], axis=1)
    mine = jnp.where(core == 0, results[:, :, :2], results[:, :, 2:])
    theirs = jnp.where(core == 0, results[:, :, 2:], results[:, :, :2])
    results = in_core_order(mine, swap(theirs), core, 3)
    results = [jnp.transpose(result, (1, 0, 2)) for result in results]

    old_other = swap(old_own)
    fields, old_own, old_other, _ = lax.optimization_barrier(
        (fields, old_own, old_other, new_line)
    )
    z = lax.axis_index("z")
    across = (chans // 2, chans)
    old_orders = [
        (ring_channel(rows_of(across, 0), which, z) == rows_of(across, 1)).astype(BF16)
        for which in (core, 1 - core)
    ]
    pulled_rows = pulled(fields, old_own, old_other, *old_orders)
    input_grad = pulled_rows.reshape(lat_rows, batch, padded_cols, chans)
    input_grad = jnp.transpose(input_grad[:, :, :lon_cols], (1, 0, 2, 3))

    rows = np.arange(chans // 4)
    back = jnp.asarray(rows[:, None] == row_channel(rows)[None, :], BF16)
    low = swap(own[: chans // 2])
    high = swap(own[chans // 2 :])
    out = joined(core_ref, back, own, low, 0, None)
    out = joined(core_ref, back, own, high, 2, out)
    new_weights = jnp.transpose(out, (1, 0, 2))
    return (input_grad, new_weights, *results)


def solution(mesh):
    split = Mesh(mesh.devices.reshape(2, 4, 8, 2, 2), ALL)
    field = P(None, LAT, LON, None)
    state = P(ALL, None, None)
    return jax.shard_map(
        per_device,
        mesh=split,
        in_specs=(field, field, state, state, state),
        out_specs=(field, P(), state, state, state, state),
        check_vma=False,
    )
```

```python
import math

import jax
import jax.numpy as jnp
import numpy as np
from jax import lax
from jax.experimental import pallas as pl
from jax.experimental.pallas import tpu as pltpu
from jax.sharding import Mesh
from jax.sharding import PartitionSpec as P


TAPS = 9
ORDER = (1, 4, 7, 0, 2, 3, 5, 6, 8)
ALL = ("xl", "y", "z", "xh", "c")
LAT = ("xl", "y")
LON = ("z", "xh", "c")
PLANE = ("xl", "y", "xh")
BF16 = jnp.bfloat16
F32 = jnp.float32

learn_rate = 0.01
beta_one = 0.9
beta_two = 0.999
adam_eps = 1e-08
decay_rate = 0.1
step_count = 10.0
norm_eps = 1e-06


def rows_of(shape, dim):
    return lax.broadcasted_iota(jnp.int32, shape, dim)


def channel_of(core, plane, z, k):
    lat, xh = plane // 2, plane % 2
    return (((lat * 8 + z) * 2 + xh) * 2 + core) * 2 + k


def ring_channel(p, core, z):
    arrival, plane, k = p // 32, (p // 2) % 16, p % 2
    step = jnp.where(arrival <= 4, -arrival, arrival - 4)
    return channel_of(core, plane, (z + step + 8) % 8, k)


def row_channel(p):
    plane, z, rest = p // 32, (p // 4) % 8, p % 4
    return channel_of(rest // 2, plane, z, rest % 2)


def neighbours(count, circular):
    forward = [(i, i + 1) for i in range(count - 1)]
    if circular:
        forward.append((count - 1, 0))
    return forward, [(b, a) for a, b in forward]


def row_halo(first, last):
    forward, backward = neighbours(8, False)
    return lax.ppermute(last, LAT, forward), lax.ppermute(first, LAT, backward)


def col_halo(parts, last_col):
    east = jnp.concatenate([part[:, :, last_col : last_col + 1] for part in parts], axis=0)
    west = jnp.concatenate([part[:, :, :1] for part in parts], axis=0)
    forward, backward = neighbours(32, True)
    return lax.ppermute(east, LON, forward), lax.ppermute(west, LON, backward)


def swap(array):
    return lax.ppermute(array, "c", [(0, 1), (1, 0)])


def store_halves(core_ref, lhs, window_of, keep_ref, send_ref):
    half = keep_ref.shape[1]
    own = pl.multiple_of(core_ref[0] * half, half)
    other = pl.multiple_of((1 - core_ref[0]) * half, half)
    send_ref[...] = window_of(lhs, pl.ds(other, half)).astype(BF16)
    keep_ref[...] = window_of(lhs, pl.ds(own, half))


def centre_kernel(core_ref, lhs_ref, above_ref, rows_ref, below_ref, keep_ref, send_ref):
    block = above_ref.shape[0]
    row = pl.program_id(0)

    def dots(pieces, outs):
        total = None
        for start, ref, first, count in pieces:
            part = jnp.dot(
                lhs_ref[:, start : start + count],
                ref[first : first + count, outs],
                preferred_element_type=F32,
            )
            total = part if total is None else total + part
        return total

    plans = (
        ((0, rows_ref, block, 3 * block), (3 * block, below_ref, 0, block)),
        ((0, rows_ref, 0, 4 * block),),
        ((0, above_ref, 0, block), (block, rows_ref, 0, 3 * block)),
    )
    for index, plan in enumerate(plans):

        @pl.when(row == index)
        def _(plan=plan):
            store_halves(core_ref, None, lambda _, outs: dots(plan, outs), keep_ref, send_ref)


def centre_grads(core, lhs, above, rows, below):
    chans, outs = lhs.shape[0], rows.shape[1]
    half = outs // 2
    whole = lambda array: pl.BlockSpec(array.shape, lambda t: (0,) * array.ndim)
    return pl.pallas_call(
        centre_kernel,
        grid=(3,),
        in_specs=[
            pl.BlockSpec(memory_space=pltpu.SMEM),
            whole(lhs),
            whole(above),
            whole(rows),
            whole(below),
        ],
        out_specs=[pl.BlockSpec((chans, half), lambda t: (0, t))] * 2,
        out_shape=[
            jax.ShapeDtypeStruct((chans, 3 * half), F32),
            jax.ShapeDtypeStruct((chans, 3 * half), BF16),
        ],
        compiler_params=pltpu.CompilerParams(vmem_limit_bytes=48 * 1024 * 1024),
        cost_estimate=pl.CostEstimate(
            flops=2 * chans * lhs.shape[1] * 3 * outs, bytes_accessed=8_000_000, transcendentals=0
        ),
        name="centre_grads",
    )(core, lhs, above, rows, below)


def side_kernel(
    core_ref, lhs_ref, above_ref, rows_ref, below_ref, left_ref, right_ref,
    field_ref, keep_ref, send_ref, *, cols, padded_cols,
):
    step = pl.program_id(0)
    block = above_ref.shape[0]
    batch = block // padded_cols

    @pl.when(step == 0)
    def _():
        index = lax.broadcasted_iota(jnp.int32, (padded_cols, 1), 0)
        for line in range(6 * batch):
            first = line * padded_cols
            if line < batch:
                ref, start = above_ref, first
            elif line < 5 * batch:
                ref, start = rows_ref, first - block
            else:
                ref, start = below_ref, first - 5 * block
            centre = ref[start : start + padded_cols, :]
            field_ref[1, first : first + padded_cols, :] = centre
            wide = centre.astype(F32)
            east = pltpu.roll(wide, padded_cols - 1, 0)
            east = jnp.where(index == cols - 1, right_ref[line // batch, line % batch].astype(F32), east)
            field_ref[0, first : first + padded_cols, :] = east.astype(BF16)
            west = pltpu.roll(wide, 1, 0)
            west = jnp.where(index == 0, left_ref[line // batch, line % batch].astype(F32), west)
            field_ref[2, first : first + padded_cols, :] = west.astype(BF16)

    row, side = step // 2, 2 * (step % 2)
    start = pl.multiple_of((2 - row) * block, block)

    def window_dot(_, outs):
        return jnp.dot(
            lhs_ref[...],
            field_ref[side, pl.ds(start, 4 * block), outs],
            preferred_element_type=F32,
        )

    store_halves(core_ref, None, window_dot, keep_ref, send_ref)


def side_grads(core, lhs, above, rows, below, left, right, cols, padded_cols):
    chans, outs = lhs.shape[0], rows.shape[1]
    half = outs // 2
    whole = lambda array: pl.BlockSpec(array.shape, lambda t: (0,) * array.ndim)
    length = rows.shape[0] * 3 // 2
    return pl.pallas_call(
        lambda *refs: side_kernel(*refs, cols=cols, padded_cols=padded_cols),
        grid=(6,),
        in_specs=[pl.BlockSpec(memory_space=pltpu.SMEM)]
        + [whole(array) for array in (lhs, above, rows, below, left, right)],
        out_specs=[pl.BlockSpec((3, length, outs), lambda t: (0, 0, 0))]
        + [pl.BlockSpec((chans, half), lambda t: (0, t))] * 2,
        out_shape=[
            jax.ShapeDtypeStruct((3, length, outs), BF16),
            jax.ShapeDtypeStruct((chans, 6 * half), F32),
            jax.ShapeDtypeStruct((chans, 6 * half), BF16),
        ],
        compiler_params=pltpu.CompilerParams(vmem_limit_bytes=56 * 1024 * 1024),
        cost_estimate=pl.CostEstimate(
            flops=2 * chans * lhs.shape[1] * 6 * outs, bytes_accessed=16_000_000, transcendentals=0
        ),
        name="side_grads",
    )(core, lhs, above, rows, below, left, right)


def pull_kernel(
    field_ref, own_ref, other_ref, own_order_ref, other_order_ref, out_ref, *, block
):
    step = pl.program_id(0)
    outs = field_ref.shape[2]
    result = None
    for weight_ref, order_ref in ((own_ref, own_order_ref), (other_ref, other_order_ref)):
        total = jnp.zeros((block, weight_ref.shape[0]), F32)
        for tap in range(TAPS):
            row, col = divmod(tap, 3)
            start = pl.multiple_of((step + 2 - row) * block, block)
            total = total + lax.dot_general(
                field_ref[col, pl.ds(start, block), :],
                weight_ref[:, tap * outs : (tap + 1) * outs],
                (((1,), (1,)), ((), ())),
                preferred_element_type=F32,
            )
        part = jnp.dot(total.astype(BF16), order_ref[...], preferred_element_type=F32)
        result = part if result is None else result + part
    out_ref[...] = result.astype(BF16)


def pulled(fields, own, other, own_order, other_order):
    block = fields.shape[1] // 6
    chans = own_order.shape[1]
    operands = (fields, own, other, own_order, other_order)
    whole = lambda array: pl.BlockSpec(array.shape, lambda i: (0,) * array.ndim)
    return pl.pallas_call(
        lambda *refs: pull_kernel(*refs, block=block),
        grid=(4,),
        in_specs=[whole(array) for array in operands],
        out_specs=pl.BlockSpec((block, chans), lambda i: (i, 0)),
        out_shape=jax.ShapeDtypeStruct((4 * block, chans), BF16),
        compiler_params=pltpu.CompilerParams(vmem_limit_bytes=48 * 1024 * 1024),
        cost_estimate=pl.CostEstimate(
            flops=2 * 4 * block * chans * own.shape[1],
            bytes_accessed=14_000_000,
            transcendentals=0,
        ),
        name="pulled",
    )(*operands)


def clip_factor(square_sum, max_norm):
    return jnp.minimum(1.0, max_norm / (jnp.sqrt(square_sum) + norm_eps))


def adam(clip, grad, master, moment_one, moment_two):
    clipped = clip * grad
    new_one = beta_one * moment_one + (1.0 - beta_one) * clipped
    new_two = beta_two * moment_two + (1.0 - beta_two) * clipped * clipped
    first_hat = new_one / (1.0 - beta_one**step_count)
    second_hat = new_two / (1.0 - beta_two**step_count)
    new_master = master - learn_rate * (
        first_hat / (jnp.sqrt(second_hat) + adam_eps) + decay_rate * master
    )
    return new_master, new_one, new_two, clipped


def join_kernel(core_ref, order_ref, own_ref, other_ref, out_ref):
    half = own_ref.shape[1] // TAPS
    own = pl.multiple_of(core_ref[0] * half, half)
    other = pl.multiple_of((1 - core_ref[0]) * half, half)
    for lane, ref in ((own, own_ref), (other, other_ref)):
        rows = jnp.dot(order_ref[...], ref[...], preferred_element_type=F32).astype(BF16)
        for index, tap in enumerate(ORDER):
            out_ref[tap, :, pl.ds(lane, half)] = rows[:, index * half : (index + 1) * half]


def joined(core, order, own, other):
    chans, wide = own.shape
    half = wide // TAPS
    block = order.shape[0]
    return pl.pallas_call(
        join_kernel,
        grid=(chans // block,),
        in_specs=[
            pl.BlockSpec(memory_space=pltpu.SMEM),
            pl.BlockSpec(order.shape, lambda i: (0, 0)),
            pl.BlockSpec((block, wide), lambda i: (i, 0)),
            pl.BlockSpec((block, wide), lambda i: (i, 0)),
        ],
        out_specs=pl.BlockSpec((TAPS, block, 2 * half), lambda i: (0, i, 0)),
        out_shape=jax.ShapeDtypeStruct((TAPS, chans, 2 * half), BF16),
        name="joined",
    )(core, order, own, other)


def around_ring(chunk, after):
    chunk, _ = lax.optimization_barrier((chunk, after))
    up = [(i, (i + 1) % 8) for i in range(8)]
    down = [(i, (i - 1) % 8) for i in range(8)]
    below, above = [chunk], [chunk]
    for _ in range(4):
        below.append(lax.ppermute(below[-1], "z", up))
    for _ in range(3):
        above.append(lax.ppermute(above[-1], "z", down))
    return jnp.concatenate(below + above[1:], axis=0)


def to_all(piece, axes, count):
    copies = jnp.broadcast_to(piece[None], (count, *piece.shape))
    return lax.all_to_all(copies, axes, 0, 0, tiled=True)


def halves(array, core):
    half = array.shape[-1] // 2
    low, high = array[..., :half], array[..., half:]
    return jnp.where(core == 0, low, high), jnp.where(core == 0, high, low)


def in_core_order(own, other, core, axis):
    return jnp.where(
        core == 0,
        jnp.concatenate([own, other], axis=axis),
        jnp.concatenate([other, own], axis=axis),
    )


def per_device(activations, upstream, master, moment_one, moment_two):
    batch, lat_rows, lon_cols, chans = activations.shape
    outs = upstream.shape[3]
    half = outs // 2
    wide = TAPS * half
    padded_cols = -(-lon_cols // 32) * 32
    extra = padded_cols - lon_cols
    core = lax.axis_index("c")
    core_ref = core.reshape(1).astype(jnp.int32)

    def padded(field):
        return jnp.pad(
            jnp.transpose(field, (1, 0, 2, 3)), ((0, 0), (0, 0), (0, extra), (0, 0))
        )

    def flat(rows):
        return rows.reshape(-1, rows.shape[3])

    above, below = row_halo(padded(upstream[:, :1]), padded(upstream[:, -1:]))
    up_rows = padded(upstream)
    rows = np.arange(chans)
    order = jnp.asarray(row_channel(rows)[:, None] == rows[None, :], BF16)
    lhs = lax.dot_general(
        order, flat(padded(activations)), (((1,), (1,)), ((), ())), preferred_element_type=F32
    ).astype(BF16)
    left, right = col_halo((above, up_rows, below), lon_cols - 1)
    pieces = (flat(above), flat(up_rows), flat(below))
    old_piece = master.astype(BF16).reshape(2, TAPS * outs)
    old_plane = to_all(old_piece, PLANE, 16).reshape(32, TAPS * outs)
    keep_one, send_one = centre_grads(core_ref, lhs, *pieces)
    swapped_one = swap(send_one)
    left, right, keep_one = lax.optimization_barrier((left, right, keep_one))
    fields, keep_two, send_two = side_grads(
        core_ref, lhs, *pieces, left, right, lon_cols, padded_cols
    )
    swapped_two = swap(send_two)
    pair_sum = jnp.concatenate(
        [
            (keep_one + swapped_one.astype(F32)).astype(BF16),
            (keep_two + swapped_two.astype(F32)).astype(BF16),
        ],
        axis=1,
    ).reshape(16, 32, wide)
    *state, pair_sum = lax.optimization_barrier((master, moment_one, moment_two, pair_sum))
    state = jnp.stack(state)
    own_state, other_state = halves(state, core)
    other_state = swap(other_state)
    state = in_core_order(own_state, other_state, core, 1)
    state = jnp.stack([state[:, :, tap] for tap in ORDER], axis=2).reshape(12, wide)
    parts = lax.all_to_all(pair_sum, PLANE, 0, 0, tiled=True)
    old_own = around_ring(old_plane, pair_sum)
    plane_sum = jnp.sum(parts.astype(F32), axis=0).astype(BF16).reshape(8, 4, wide)
    parts = lax.all_to_all(plane_sum, ("z",), 0, 0, tiled=True)
    grad = jnp.sum(parts.astype(F32), axis=0)

    square_sum = jnp.sum(grad * grad).reshape(1, 1)
    square_sum = square_sum + swap(square_sum)
    square_sum = jnp.sum(to_all(square_sum, ("xl", "y", "z", "xh"), 128)).reshape(1, 1)
    clip = clip_factor(square_sum, math.sqrt(float(chans * TAPS * outs)))
    results = jnp.stack(adam(clip, grad, *state.reshape(3, 4, wide)))
    new_line = to_all(results[0].astype(BF16), ("z",), 8).reshape(32, wide)
    own = to_all(new_line, PLANE, 16).reshape(chans, wide)

    results = results.reshape(4, 4, TAPS, half)
    results = jnp.stack([results[:, :, ORDER.index(tap)] for tap in range(TAPS)], axis=1)
    mine = jnp.where(core == 0, results[:, :, :2], results[:, :, 2:])
    theirs = jnp.where(core == 0, results[:, :, 2:], results[:, :, :2])
    results = in_core_order(mine, swap(theirs), core, 3)
    results = [jnp.transpose(result, (1, 0, 2)) for result in results]

    old_other = swap(old_own)
    fields, old_own, old_other, _ = lax.optimization_barrier(
        (fields, old_own, old_other, new_line)
    )
    z = lax.axis_index("z")
    across = (chans // 2, chans)
    old_orders = [
        (ring_channel(rows_of(across, 0), which, z) == rows_of(across, 1)).astype(BF16)
        for which in (core, 1 - core)
    ]
    pulled_rows = pulled(fields, old_own, old_other, *old_orders)
    input_grad = pulled_rows.reshape(lat_rows, batch, padded_cols, chans)
    input_grad = jnp.transpose(input_grad[:, :, :lon_cols], (1, 0, 2, 3))

    rows = np.arange(chans // 2)
    back = jnp.asarray(rows[:, None] == row_channel(rows)[None, :], BF16)
    out = joined(core_ref, back, own, swap(own))
    new_weights = jnp.transpose(out, (1, 0, 2))
    return (input_grad, new_weights, *results)


def solution(mesh):
    split = Mesh(mesh.devices.reshape(2, 4, 8, 2, 2), ALL)
    field = P(None, LAT, LON, None)
    state = P(ALL, None, None)
    return jax.shard_map(
        per_device,
        mesh=split,
        in_specs=(field, field, state, state, state),
        out_specs=(field, P(), state, state, state, state),
        check_vma=False,
    )
```
